32 devices in a mesh: batch: 8 (over y, x, core), head: 4 (over z).
Axes of the slice: x: 2, y: 2, z: 4, core: 2. Of those that a mesh axis runs over, the one named last changes fastest.
Arguments:
- inputs: bfloat16 [8, 128, 2048], P(None, 'batch', 'head'), parts along dimension 1, may hold values from -6 to 6
- in_weight: bfloat16 [2048, 4, 384], P(None, 'head'), may hold values from -0.125 to 0.125
- gate_weight: bfloat16 [2048, 4], P(None, 'head'), may hold values from -0.125 to 0.125
- gate_bias: float32 [4], P('head'), may hold values from -2 to 3
- norm_gain: float32 [512], P('head'), may hold values from 0.1 to 1.9
- out_weight: bfloat16 [512, 2048], P('head'), may hold values from -0.375 to 0.375
- inv_gram: float32 [128, 4, 128, 128], P('batch', 'head'), parts along dimension 0, may hold values from -17 to 17, as said below
- value_key: float32 [128, 4, 128, 128], P('batch', 'head'), parts along dimension 0, may hold values from -6 to 6
Outputs:
- layer_out: float32 [8, 128, 2048], P(None, 'batch', 'head'), parts along dimension 1
The draws below stay inside these ranges and needn't reach their ends.
There are 8 independent parts, one for each index of `batch`. The reference program is written for one: setup_inputs(seed, part) draws one part's arguments, and reference() takes and returns one part's arrays. A program takes and returns all parts, laid end to end along the dimension named above; an argument that names none is the same for every part. Nothing has to cross between parts.
Inputs may be any that keep to these rules, and one draw needn't show every extreme that they name: `inv_gram`: each [128, 128] matrix is symmetric positive definite.
All inputs are finite; a program needn't handle non-finite values.
Results may differ from the reference program's by a relative error of at most 0.0029.
Values may be sent and summed in bfloat16 or wider, within the bound.
A program may use at most 64 MiB of HBM per device.

```python
import jax
import jax.numpy as jnp
from jax import lax

D = 2048
DH = 128
SEQS = 16
STEPS = 8
HEADS = 4


def draw_inv_gram(key, part):
    shape = (SEQS, HEADS, DH, DH)
    entries = jnp.clip(jax.random.normal(key, shape, jnp.float32), -4.0, 4.0)
    gram_part = jnp.einsum('shij,shkj->shik', entries, entries, precision=lax.Precision.HIGHEST) / DH
    return 0.5 * jnp.eye(DH, dtype=jnp.float32) + gram_part


def draw_value_key(key, part):
    shape = (SEQS, HEADS, DH, DH)
    rising = 3.0 ** (jnp.arange(HEADS, dtype=jnp.float32) / max(HEADS - 1, 1))
    entries = jnp.clip(jax.random.normal(key, shape, jnp.float32), -4.0, 4.0)
    scales = 0.12 * jnp.broadcast_to(rising[None, :], (SEQS, HEADS))
    return entries * scales[:, :, None, None]


def raised(values, key, source, target, blocks, factor):
    owner, partner = [(jnp.arange(values.shape[dim]) // (values.shape[dim] // blocks)).reshape([-1 if axis == dim else 1 for axis in range(values.ndim)]) for dim in (source, target)]
    chosen = jax.random.permutation(key, blocks)[partner]
    strong = (owner == chosen) | (owner == (partner + blocks // 2) % blocks)
    return jnp.where(strong, factor * values, values)


def steps_of(rng, shape, split, low, high):
    loudness = 1.0
    for dim, shards_of in split:
        draws = jax.random.uniform(jax.random.fold_in(jax.random.fold_in(rng, 6), dim), (shards_of,), jnp.float32, low / len(split), high / len(split))
        loudness = loudness * jnp.repeat(jnp.exp(draws), shape[dim] // shards_of).reshape((-1,) + (1,) * (len(shape) - 1 - dim))
    return loudness


def normal_values(own_key, extent, spread, reach, cuts=(), kind=jnp.bfloat16):
    loudness = steps_of(own_key, extent, cuts, -0.22, 0.18) if cuts else 1.0
    array = jax.random.normal(own_key, extent, jnp.float32) * spread * loudness
    return jnp.minimum(jnp.maximum(array, -reach), reach).astype(kind)


def heavy_noise(rng, dims, width, reach, shards, heavy, kind=jnp.bfloat16):
    values = width * jax.random.normal(rng, dims, jnp.float32)
    if shards:
        values = values * steps_of(rng, dims, shards, -0.22, 0.18)
    return jnp.clip(raised(values, jax.random.fold_in(rng, 3), *heavy), -reach, reach).astype(kind)


def setup_inputs(seed: int = 0, part: int = 0) -> dict:
    splits = jax.random.split(jax.random.key(seed), 9)
    part_splits = jax.random.split(jax.random.fold_in(splits[8], part), 9)
    inputs = normal_values(part_splits[0], (STEPS, SEQS, D), 1.0, 6.0, ((2, 4),))
    in_weight = normal_values(splits[1], (D, HEADS, 3 * DH), D ** -0.5, 0.125, ((1, 4),))
    gate_weight = normal_values(splits[2], (D, HEADS), D ** -0.5, 0.125, ((1, 4),))
    gate_bias = jnp.clip(-2.0 + 5.0 * jax.random.uniform(splits[3], (HEADS,), jnp.float32) ** steps_of(splits[3], (HEADS,), ((0, 4),), -0.2, 0.2), -2.0, 3.0)
    norm_gain = jnp.clip(1.0 + 0.18 * jax.random.normal(splits[4], (HEADS * DH,), jnp.float32), 0.1, 1.9)
    out_weight = heavy_noise(splits[5], (HEADS * DH, D), (HEADS * DH) ** -0.5, 0.375, ((0, 4),), (0, 1, 4, 2.0))
    inv_gram = draw_inv_gram(jax.random.fold_in(jax.random.fold_in(splits[8], part), 71), part)
    value_key = draw_value_key(jax.random.fold_in(jax.random.fold_in(splits[8], part), 71), part)
    return dict(inputs=inputs, in_weight=in_weight, gate_weight=gate_weight, gate_bias=gate_bias, norm_gain=norm_gain, out_weight=out_weight, inv_gram=inv_gram, value_key=value_key)


def advance(gram_inv, memory, projected, gate, gate_bias, head_size):
    batch_rows, local_heads = gate.shape
    pieces = projected.reshape(batch_rows, local_heads, 3 * head_size)
    queries = pieces[..., :head_size]
    keys_now = pieces[..., head_size:2 * head_size]
    values_now = pieces[..., 2 * head_size:]
    forget = 0.8 + 0.2 * jax.nn.sigmoid(gate + gate_bias)
    keys_now = keys_now * lax.rsqrt(lax.optimization_barrier(jnp.sum(keys_now * keys_now, axis=-1, keepdims=True)) + 1e-06)
    queries = queries * lax.rsqrt(lax.optimization_barrier(jnp.sum(queries * queries, axis=-1, keepdims=True)) + 1e-06)
    gram_key = jnp.einsum('bhij,bhj->bhi', gram_inv, keys_now, precision=lax.Precision.HIGHEST)
    denominator = forget + lax.optimization_barrier(jnp.sum(keys_now * gram_key, axis=-1))
    gram_inv = (gram_inv - gram_key[..., :, None] * gram_key[..., None, :] / denominator[..., None, None]) / forget[..., None, None]
    memory = forget[..., None, None] * memory + values_now[..., :, None] * keys_now[..., None, :]
    gram_query = jnp.einsum('bhij,bhj->bhi', gram_inv, queries, precision=lax.Precision.HIGHEST)
    readout = jnp.einsum('bhij,bhj->bhi', memory, gram_query, precision=lax.Precision.HIGHEST)
    return (gram_inv, memory, readout.reshape(batch_rows, local_heads * head_size))

def reference(inputs, in_weight, gate_weight, gate_bias, norm_gain, out_weight, inv_gram, value_key):
    weight_flat = in_weight.reshape(D, HEADS * 3 * DH)
    gram_inv = inv_gram
    memory = value_key
    results = []
    for position in range(STEPS):
        projected = jnp.dot(inputs[position], weight_flat, preferred_element_type=jnp.float32)
        gate = jnp.dot(inputs[position], gate_weight, preferred_element_type=jnp.float32)
        gram_inv, memory, readout = advance(gram_inv, memory, projected, gate, gate_bias, DH)
        mean_square = lax.optimization_barrier(jnp.mean(readout * readout, axis=-1))
        hidden = (norm_gain * readout * lax.rsqrt(mean_square + 1e-06)[:, None]).astype(jnp.bfloat16)
        results.append(jnp.dot(hidden, out_weight, preferred_element_type=jnp.float32))
    return jnp.stack(results, axis=0)
```

```python
import functools
import math

import jax
import jax.numpy as jnp
from jax import lax
from jax.experimental import pallas as pl
from jax.experimental.pallas import tpu as pltpu
from jax.sharding import PartitionSpec as P

MESH = pl.DeviceIdType.MESH
F32 = jnp.float32
BF16 = jnp.bfloat16
NT = (((1,), (1,)), ((), ()))
PIECES = 4
GROUPS = ((0, 1), (2, 3))


def split(x):
    hi = x.astype(BF16)
    lo = (x - hi.astype(F32)).astype(BF16)
    return hi, lo


def rowsum(x):
    return jnp.sum(x, axis=-1, keepdims=True)


def select(me, values):
    out = jnp.int32(values[0])
    for m in range(1, len(values)):
        out = jnp.where(me == m, jnp.int32(values[m]), out)
    return out


def arrivals(n, groups, width):
    out = []
    for m in range(n):
        found = []
        for j in range(n):
            for g in range(groups):
                hops = abs(j - m)
                late = 3.0 if j > m else 0.0
                found.append(((hops - 1) * groups * width + (g + 1) * width + 2.4 * hops + late, j, g))
        out.append([(j, g) for _, j, g in sorted(found) if j != m])
    return out


def kernel(
    n,
    group,
    x_hbm,
    w_hbm,
    gate_hbm,
    bias_hbm,
    gain_hbm,
    ow_hbm,
    a_hbm,
    m_hbm,
    out_ref,
    bias_ref,
    gain_ref,
    xg,
    w,
    gate,
    a32,
    m32,
    ab,
    wout,
    pacc,
    gacc,
    kq,
    abuf,
    bbuf,
    rbuf,
    sqbuf,
    lsem,
    xr,
    know,
    w1r,
    chip_r,
    core_r,
    early_r,
    rr,
    sent,
):
    steps, seqs, feats = x_hbm.shape
    rows = steps * seqs
    heads_rows = ow_hbm.shape[0]
    cols = ow_hbm.shape[1] // n
    size = a_hbm.shape[1]
    me = lax.axis_index("head")
    b = lax.axis_index("batch")
    mine = lax.rem(b, group)
    base = b - mine
    slab = heads_rows // group
    has_left = me > 0
    has_right = me < n - 1

    parity = lax.rem(mine, 2)
    chip = lax.div(mine, 2)
    chips = group // 2
    bits = chips.bit_length() - 1

    def flip(value, bit):
        return value + (1 - 2 * lax.rem(lax.div(value, 1 << bit), 2)) * (1 << bit)

    core_peer = base + mine + 1 - 2 * parity
    near = [base + 2 * flip(chip, bit) + parity for bit in range(bits)]
    place = parity * chips + chip

    barrier = pltpu.get_barrier_semaphore()

    @pl.when(has_left)
    def _():
        pl.semaphore_signal(barrier, inc=1, device_id={"head": me - 1}, device_id_type=MESH)

    @pl.when(has_right)
    def _():
        pl.semaphore_signal(barrier, inc=1, device_id={"head": me + 1}, device_id_type=MESH)

    for peer in [core_peer] + near:
        pl.semaphore_signal(barrier, inc=1, device_id={"batch": peer}, device_id_type=MESH)

    loads = [
        pltpu.make_async_copy(x_hbm, xg.at[me], lsem.at[0]),
        pltpu.make_async_copy(w_hbm, w, lsem.at[1]),
        pltpu.make_async_copy(gate_hbm, gate, lsem.at[1]),
        pltpu.make_async_copy(a_hbm, a32, lsem.at[1]),
        pltpu.make_async_copy(m_hbm, m32, lsem.at[1]),
        pltpu.make_async_copy(
            ow_hbm.at[:, pl.ds(pl.multiple_of(me * cols, cols), cols)], wout.at[me], lsem.at[1]
        ),
        pltpu.make_async_copy(bias_hbm, bias_ref, lsem.at[1]),
        pltpu.make_async_copy(gain_hbm, gain_ref, lsem.at[1]),
    ]
    for load in loads:
        load.start()

    order = [sorted((j for j in range(n) if j != m), key=lambda j: (abs(j - m), j)) for m in range(n)]
    sources = [select(me, [order[m][k] for m in range(n)]) for k in range(n - 1)]
    span = steps // PIECES

    groups = len(GROUPS)
    width = len(GROUPS[0])
    slots = arrivals(n, groups, width)
    slot_block = [select(me, [slots[m][k][0] for m in range(n)]) for k in range(len(slots[0]))]
    slot_group = [select(me, [slots[m][k][1] for m in range(n)]) for k in range(len(slots[0]))]
    early = max(k + 1 for m in range(n) for k, (_, g) in enumerate(slots[m]) if g == 0)

    def slot_of(j, receiver):
        return j - (j > receiver).astype(jnp.int32)

    def xcopy(side, j, c):
        part = xg.at[j, pl.ds(c * span, span)]
        peer = me + 2 * side - 1
        return pltpu.make_async_remote_copy(
            src_ref=part,
            dst_ref=part,
            send_sem=sent,
            recv_sem=xr.at[slot_of(j, peer), c],
            device_id={"head": peer},
            device_id_type=MESH,
        )

    def landed(part, sem):
        pltpu.make_async_remote_copy(
            src_ref=part,
            dst_ref=part,
            send_sem=sent,
            recv_sem=sem,
            device_id={"head": me},
            device_id_type=MESH,
        ).wait_recv()

    loads[0].wait()
    with jax.named_scope("barrier"):
        pl.semaphore_wait(barrier, has_left.astype(jnp.int32) + has_right.astype(jnp.int32) + 1 + bits)

    @pl.when(has_right)
    def _():
        for c in GROUPS[0]:
            xcopy(1, me, c).start()

    def send_rest():
        for c in range(width, PIECES):
            xcopy(1, me, c).start()

    @pl.when(has_right & (parity == 0))
    def _():
        send_rest()

    @pl.when(has_left)
    def _():
        for c in range(PIECES):
            xcopy(0, me, c).start()

    with jax.named_scope("know"):
        for d in range(2, n):

            @pl.when((me >= d - 1) & has_right)
            def _():
                pl.semaphore_signal(know.at[0], inc=1, device_id={"head": me + 1}, device_id_type=MESH)

            @pl.when(me >= d)
            def _():
                pl.semaphore_wait(know.at[0], 1)

        if bits == 2:
            pl.semaphore_signal(know.at[2], inc=1, device_id={"batch": near[0]}, device_id_type=MESH)

    def tell_left(d):
        @pl.when((me + d - 1 < n) & has_left)
        def _():
            pl.semaphore_signal(know.at[1], inc=1, device_id={"head": me - 1}, device_id_type=MESH)

    def hear_right(d):
        @pl.when(me + d < n)
        def _():
            pl.semaphore_wait(know.at[1], 1)

    if n > 2:
        tell_left(2)

    def w1copy(j):
        at = pl.ds(pl.multiple_of(place * slab, slab), slab)
        return pltpu.make_async_remote_copy(
            src_ref=ow_hbm.at[at, pl.ds(pl.multiple_of(j * cols, cols), cols)],
            dst_ref=wout.at[me, at],
            send_sem=sent,
            recv_sem=w1r,
            device_id={"head": j},
            device_id_type=MESH,
        )

    def w2copy(j, peer, sem, rows_sent, begin):
        part = wout.at[j, pl.ds(pl.multiple_of(begin, slab), rows_sent)]
        return pltpu.make_async_remote_copy(
            src_ref=part,
            dst_ref=part,
            send_sem=sent,
            recv_sem=sem,
            device_id={"batch": peer},
            device_id_type=MESH,
        )

    def chip_copies(j):
        return [
            w2copy(j, base + 2 * lax.rem(chip + o, chips) + parity, chip_r, slab, place * slab)
            for o in range(1, chips)
        ]

    def core_copy(j):
        return w2copy(j, core_peer, core_r, chips * slab, parity * chips * slab)

    def spread_chips():
        if bits == 2:
            pl.semaphore_wait(know.at[2], 1)
        landed(wout.at[: n - 1, :slab], w1r)
        for j in sources:
            for copy in chip_copies(j):
                copy.start()

    def spread_cores():
        landed(wout.at[: n - 1, : (chips - 1) * slab], chip_r)
        for j in sources:
            core_copy(j).start()

    def project(j, begin, count, first):
        x = xg[j, pl.ds(begin, count)].reshape(count * seqs, feats)
        at = pl.ds(pl.multiple_of(j * feats, feats), feats)
        part = jnp.dot(x, w[at, :], preferred_element_type=F32)
        g = jnp.broadcast_to(gate[:, at].astype(F32), (size, feats)).astype(BF16)
        gpart = lax.dot_general(x, g, NT, preferred_element_type=F32)
        at = pl.ds(pl.multiple_of(begin * seqs, seqs), count * seqs)
        if first:
            pacc[at, :] = part
            gacc[at, :] = gpart
        else:
            pacc[at, :] += part
            gacc[at, :] += gpart

    def prepare(start, stop):
        for s in range(start, stop):
            ah, al = split(a32[s])
            mh, ml = split(m32[s])
            bt = lax.dot_general(
                jnp.concatenate([ah, al], axis=1),
                jnp.concatenate([mh, mh], axis=1),
                NT,
                preferred_element_type=F32,
            )
            bt = bt + lax.dot_general(ah, ml, NT, preferred_element_type=F32)
            bh, bl = split(bt)
            ab[s, :size, :size] = ah
            ab[s, size:, :size] = al
            ab[s, :size, size:] = bh
            ab[s, size:, size:] = bl

    for j in sources:

        @pl.when(j < me)
        def _():
            w1copy(j).start()

    with jax.named_scope("proj0"):
        for load in loads[1:]:
            load.wait()
        project(me, 0, steps, True)
    with jax.named_scope("prepA"):
        prepare(0, seqs // 2)

    @pl.when(has_right & (parity == 1))
    def _():
        send_rest()

    @pl.when(me + 1 < n - 1)
    def _():
        w1copy(me + 1).start()

    def collect(begin, end):
        for k in range(begin, end):
            j, g = slot_block[k], slot_group[k]
            for at in range(width):
                c = g * width + at
                with jax.named_scope("x%d_%d" % (k, at)):
                    landed(xg.at[j, pl.ds(c * span, span)], xr.at[slot_of(j, me), c])

                @pl.when((j < me) & has_right)
                def _():
                    xcopy(1, j, c).start()

                @pl.when((j > me) & has_left)
                def _():
                    xcopy(0, j, c).start()

            with jax.named_scope("p%d" % k):
                project(j, g * width * span, width * span, False)
            if k < early:
                half = seqs // 2
                prepare(half + half * k // early, half + half * (k + 1) // early)

    past = []
    product = [None]

    def outgoing(part, j, sem):
        return pltpu.make_async_remote_copy(
            src_ref=part,
            dst_ref=part,
            send_sem=sent,
            recv_sem=sem,
            device_id={"head": j},
            device_id_type=MESH,
        )

    def rcopies(j, g):
        sem = rr.at[slot_of(me, j)] if g == groups - 1 else early_r.at[g]
        begin, end = g * width * span * seqs, (g + 1) * width * span * seqs
        return [
            outgoing(rbuf.at[me, pl.ds(begin, end - begin)], j, sem),
            outgoing(sqbuf.at[g, me], j, sem),
        ]

    def advance(g):
        first, last = GROUPS[g][0] * span, (GROUPS[g][-1] + 1) * span
        count = last - first
        half = count * seqs
        at = slice(first * seqs, last * seqs)
        p = pacc[at, :]
        f = 0.8 + 0.2 * jax.nn.sigmoid(gacc[at, :] + bias_ref[...])
        q = p[:, :size]
        k = p[:, size : 2 * size]
        v = p[:, 2 * size :]
        k = k * lax.rsqrt(rowsum(k * k) + 1e-06)
        q = q * lax.rsqrt(rowsum(q * q) + 1e-06)
        kq[:half, :] = k
        kq[half : 2 * half, :] = q
        for s in range(seqs):
            at = pl.ds(s, 2 * count, stride=seqs)
            hi, lo = split(kq[at, :])
            left = jnp.concatenate([hi.astype(F32), lo.astype(F32)], axis=0).astype(BF16)
            r = jnp.dot(jnp.concatenate([left, left], axis=1), ab[s], preferred_element_type=F32)
            r = r[: 2 * count] + r[2 * count :]
            abuf[at, :] = r[:, :size]
            bbuf[at, :] = r[:, size:]

        def piece(x, t):
            return x[t * seqs : (t + 1) * seqs]

        kt = [piece(k, t) for t in range(count)]
        qt = [piece(q, t) for t in range(count)]
        a = [u for u, _, _, _ in past] + [piece(abuf, t) for t in range(count)]
        dots = [[rowsum(a[s] * kt[t]) for s in range(first + t + 1)] for t in range(count)]
        reads = [[rowsum(a[s] * qt[t]) for s in range(first + t + 1)] for t in range(count)]
        pieces = []
        for t in range(count):
            ft = piece(f, t)
            product[0] = ft if product[0] is None else product[0] * ft
            now = first + t
            for s in range(now + 1):
                lower = past[s][1] if s < now else [past[r][2] * dots[t][r] for r in range(now)]
                for r in range(s):
                    dots[t][s] = dots[t][s] - lower[r] * dots[t][r]
                    reads[t][s] = reads[t][s] - lower[r] * reads[t][r]
            weight = 1.0 / (product[0] + dots[t][now])
            value = piece(v, t) - piece(bbuf, t)
            for s in range(now):
                value = value - dots[t][s] * past[s][3]
            past.append((a[now], [past[r][2] * dots[t][r] for r in range(now)], weight, weight * value))
            total = piece(bbuf, count + t)
            for s in range(now + 1):
                total = total + reads[t][s] * past[s][3]
            pieces.append(total)
        ro = jnp.concatenate(pieces, axis=0)
        hi, lo = split(ro * ro)
        both = jnp.concatenate([hi, lo], axis=1)
        sqbuf[g, me] = lax.dot_general(
            jnp.ones((8, 2 * size), BF16),
            jnp.concatenate([both] * (rows // half), axis=0),
            NT,
            preferred_element_type=F32,
        )
        rbuf[me, first * seqs : last * seqs] = (gain_ref[...] * ro).astype(BF16)
        for j in reversed(sources):
            for copy in rcopies(j, g):
                copy.start()

    inner = has_left & has_right
    collect(0, 1)
    if n > 2:
        hear_right(2)
        if n > 3:
            tell_left(3)
    collect(1, 2)
    with jax.named_scope("learn"):
        for d in range(3, n):
            hear_right(d)
            if d + 1 < n:
                tell_left(d + 1)

    for j in sources:

        @pl.when((j > me + 1) & ((j < n - 1) | (me == 0)))
        def _():
            w1copy(j).start()

    collect(2, early - 1)
    with jax.named_scope("spreadA0"):

        @pl.when(me == 0)
        def _():
            spread_chips()

    @pl.when(inner & (me < n - 2))
    def _():
        w1copy(n - 1).start()

    collect(early - 1, early)

    @pl.when(inner)
    def _():
        collect(early, len(slot_block))

    @pl.when((me == n - 2) | ((me == 0) & (n == 2)))
    def _():
        w1copy(n - 1).start()

    with jax.named_scope("spreadA1"):

        @pl.when(inner)
        def _():
            spread_chips()

    with jax.named_scope("adv0"):
        advance(0)

    @pl.when(jnp.logical_not(inner))
    def _():
        collect(early, len(slot_block))

    @pl.when(me == n - 1)
    def _():
        spread_chips()

    with jax.named_scope("adv1"):
        advance(1)

    with jax.named_scope("spreadB"):
        spread_cores()

    def send_done(part):
        pltpu.make_async_remote_copy(
            src_ref=part,
            dst_ref=part,
            send_sem=sent,
            recv_sem=w1r,
            device_id={"head": me},
            device_id_type=MESH,
        ).wait_send()

    with jax.named_scope("spreadC"):
        landed(wout.at[: n - 1, : chips * slab], core_r)

    def finish(g):
        part = slice(g * width * span * seqs, (g + 1) * width * span * seqs)
        count = width * span * seqs
        acc = jnp.dot(rbuf[me, part], wout[me], preferred_element_type=F32)
        squares = sqbuf[g, me]
        extra = 8 * rows * 4 // (size * 2)
        if g < groups - 1:
            landed(rbuf.at[: n - 1, : count + extra], early_r.at[g])
        for k, j in enumerate(sources):
            if g == groups - 1:
                with jax.named_scope("r%d" % k):
                    landed(rbuf.at[j, : count + extra], rr.at[slot_of(j, me)])
            acc = acc + jnp.dot(rbuf[j, part], wout[j], preferred_element_type=F32)
            squares = squares + sqbuf[g, j]
        scale = lax.rsqrt(squares[:1] / (n * size) + 1e-06)
        scale = jnp.broadcast_to(scale, (size, rows)).T[:count]
        for at in range(0, cols, size):
            out_ref[part, at : at + size] = acc[:, at : at + size] * scale

    for g in range(groups):
        if g == groups - 1:
            with jax.named_scope("sends"):
                @pl.when(has_right)
                def _():
                    send_done(xg.at[0])

                @pl.when(has_left)
                def _():
                    send_done(xg.at[0])

                for j in sources:

                    @pl.when(inner)
                    def _():
                        send_done(xg.at[0])

                for j in sources:
                    send_done(wout.at[0, :slab])
                    send_done(wout.at[0, : (chips - 1) * slab])
                    send_done(wout.at[0, : chips * slab])
                    for copy in rcopies(j, 0):
                        copy.wait_send()
        with jax.named_scope("finish%d" % g):
            finish(g)

    for j in sources:
        for copy in rcopies(j, groups - 1):
            copy.wait_send()


def local(n, batch, inputs, in_weight, gate_weight, gate_bias, norm_gain, out_weight, inv_gram, value_key):
    steps, seqs, feats = inputs.shape
    d_model, heads, width = in_weight.shape
    size = width // 3
    rows = steps * seqs
    cols = out_weight.shape[1] // n
    group = math.gcd(math.gcd(batch, 8), out_weight.shape[0] // 16)
    assert heads == 1 and steps % PIECES == 0 and group > 1
    anywhere = pl.BlockSpec(memory_space=pl.ANY)
    vmem = pl.BlockSpec(memory_space=pltpu.VMEM)
    dma = pltpu.SemaphoreType.DMA
    out = pl.pallas_call(
        functools.partial(kernel, n, group),
        out_shape=pltpu.VMEM((rows, cols), F32),
        in_specs=[anywhere] * 8,
        out_specs=vmem,
        scratch_shapes=[
            pltpu.VMEM((1, 1), F32),
            pltpu.VMEM((1, size), F32),
            pltpu.VMEM((n, steps, seqs, feats), BF16),
            pltpu.VMEM((d_model, width), BF16),
            pltpu.VMEM((1, d_model), BF16),
            pltpu.VMEM((seqs, size, size), F32),
            pltpu.VMEM((seqs, size, size), F32),
            pltpu.VMEM((seqs, 2 * size, 2 * size), BF16),
            pltpu.VMEM((n, out_weight.shape[0], cols), BF16),
            pltpu.VMEM((rows, width), F32),
            pltpu.VMEM((rows, size), F32),
            pltpu.VMEM((2 * rows, size), F32),
            pltpu.VMEM((2 * rows, size), F32),
            pltpu.VMEM((2 * rows, size), F32),
            pltpu.VMEM((n, rows, size), BF16),
            pltpu.VMEM((len(GROUPS), n, 8, rows), F32),
            dma((2,)),
            dma((n - 1, PIECES)),
            pltpu.SemaphoreType.REGULAR((3,)),
            dma,
            dma,
            dma,
            dma((len(GROUPS) - 1,)),
            dma((n - 1,)),
            dma,
        ],
        compiler_params=pltpu.CompilerParams(collective_id=0, has_side_effects=True),
    )(
        inputs,
        in_weight.reshape(d_model, width),
        gate_weight.reshape(1, d_model),
        gate_bias.reshape(1, 1),
        norm_gain.reshape(1, size),
        out_weight,
        inv_gram.reshape(seqs, size, size),
        value_key.reshape(seqs, size, size),
    )
    return out.reshape(steps, seqs, cols)


def solution(mesh):
    in_specs = (
        P(None, "batch", "head"),
        P(None, "head", None),
        P(None, "head"),
        P("head"),
        P("head"),
        P("head", None),
        P("batch", "head", None, None),
        P("batch", "head", None, None),
    )
    out_specs = P(None, "batch", "head")
    return jax.shard_map(
        functools.partial(local, mesh.shape["head"], mesh.shape["batch"]),
        mesh=mesh,
        in_specs=in_specs,
        out_specs=out_specs,
        check_vma=False,
    )
```

```python
import functools
import math

import jax
import jax.numpy as jnp
from jax import lax
from jax.experimental import pallas as pl
from jax.experimental.pallas import tpu as pltpu
from jax.sharding import PartitionSpec as P

MESH = pl.DeviceIdType.MESH
F32 = jnp.float32
BF16 = jnp.bfloat16
NT = (((1,), (1,)), ((), ()))
PIECES = 4
GROUPS = ((0, 1), (2, 3))


def split(x):
    hi = x.astype(BF16)
    lo = (x - hi.astype(F32)).astype(BF16)
    return hi, lo


def rowsum(x):
    return jnp.sum(x, axis=-1, keepdims=True)


def select(me, values):
    out = jnp.int32(values[0])
    for m in range(1, len(values)):
        out = jnp.where(me == m, jnp.int32(values[m]), out)
    return out


def arrivals(n, groups, width):
    out = []
    for m in range(n):
        found = []
        for j in range(n):
            for g in range(groups):
                hops = abs(j - m)
                late = 0.0 if j < m else 1.7 if j == n - 1 and hops == 1 else 3.0
                found.append(((hops - 1) * groups * width + (g + 1) * width + 2.4 * hops + late, j, g))
        out.append([(j, g) for _, j, g in sorted(found) if j != m])
    return out


def kernel(
    n,
    group,
    x_hbm,
    w_hbm,
    gate_hbm,
    bias_hbm,
    gain_hbm,
    ow_hbm,
    a_hbm,
    m_hbm,
    out_ref,
    bias_ref,
    gain_ref,
    xg,
    w,
    gate,
    a32,
    m32,
    ab,
    wout,
    pacc,
    gacc,
    kq,
    abuf,
    bbuf,
    rbuf,
    sqbuf,
    lsem,
    xr,
    know,
    turn,
    w1r,
    chip_r,
    core_r,
    early_r,
    rr,
    sent,
):
    steps, seqs, feats = x_hbm.shape
    rows = steps * seqs
    heads_rows = ow_hbm.shape[0]
    cols = ow_hbm.shape[1] // n
    size = a_hbm.shape[1]
    me = lax.axis_index("head")
    b = lax.axis_index("batch")
    mine = lax.rem(b, group)
    base = b - mine
    has_left = me > 0
    has_right = me < n - 1

    parity = lax.rem(mine, 2)
    chip = lax.div(mine, 2)
    chips = group // 2
    bits = chips.bit_length() - 1

    def flip(value, bit):
        return value + (1 - 2 * lax.rem(lax.div(value, 1 << bit), 2)) * (1 << bit)

    core_peer = base + mine + 1 - 2 * parity
    near = [base + 2 * flip(chip, bit) + parity for bit in range(bits)]
    slab = heads_rows // chips
    spreads = parity == 1

    barrier = pltpu.get_barrier_semaphore()

    @pl.when(has_left)
    def _():
        pl.semaphore_signal(barrier, inc=1, device_id={"head": me - 1}, device_id_type=MESH)

    @pl.when(has_right)
    def _():
        pl.semaphore_signal(barrier, inc=1, device_id={"head": me + 1}, device_id_type=MESH)

    pl.semaphore_signal(barrier, inc=1, device_id={"batch": core_peer}, device_id_type=MESH)

    @pl.when(spreads)
    def _():
        for peer in near:
            pl.semaphore_signal(barrier, inc=1, device_id={"batch": peer}, device_id_type=MESH)

    loads = [
        pltpu.make_async_copy(x_hbm, xg.at[me], lsem.at[0]),
        pltpu.make_async_copy(w_hbm, w, lsem.at[1]),
        pltpu.make_async_copy(gate_hbm, gate, lsem.at[1]),
        pltpu.make_async_copy(a_hbm, a32, lsem.at[1]),
        pltpu.make_async_copy(m_hbm, m32, lsem.at[1]),
        pltpu.make_async_copy(
            ow_hbm.at[:, pl.ds(pl.multiple_of(me * cols, cols), cols)], wout.at[me], lsem.at[1]
        ),
        pltpu.make_async_copy(bias_hbm, bias_ref, lsem.at[1]),
        pltpu.make_async_copy(gain_hbm, gain_ref, lsem.at[1]),
    ]
    for load in loads:
        load.start()

    order = [sorted((j for j in range(n) if j != m), key=lambda j: (abs(j - m), j)) for m in range(n)]
    sources = [select(me, [order[m][k] for m in range(n)]) for k in range(n - 1)]
    span = steps // PIECES

    groups = len(GROUPS)
    width = len(GROUPS[0])
    slots = arrivals(n, groups, width)
    slot_block = [select(me, [slots[m][k][0] for m in range(n)]) for k in range(len(slots[0]))]
    slot_group = [select(me, [slots[m][k][1] for m in range(n)]) for k in range(len(slots[0]))]
    early = max(k + 1 for m in range(n) for k, (_, g) in enumerate(slots[m]) if g == 0)

    def slot_of(j, receiver):
        return j - (j > receiver).astype(jnp.int32)

    def xcopy(side, j, c):
        part = xg.at[j, pl.ds(c * span, span)]
        peer = me + 2 * side - 1
        return pltpu.make_async_remote_copy(
            src_ref=part,
            dst_ref=part,
            send_sem=sent,
            recv_sem=xr.at[slot_of(j, peer), c],
            device_id={"head": peer},
            device_id_type=MESH,
        )

    def landed(part, sem):
        pltpu.make_async_remote_copy(
            src_ref=part,
            dst_ref=part,
            send_sem=sent,
            recv_sem=sem,
            device_id={"head": me},
            device_id_type=MESH,
        ).wait_recv()

    loads[0].wait()
    with jax.named_scope("barrier"):
        pl.semaphore_wait(barrier, has_left.astype(jnp.int32) + has_right.astype(jnp.int32) + 1 + bits * parity)

    @pl.when(has_right)
    def _():
        for c in GROUPS[0]:
            xcopy(1, me, c).start()

    def send_rest():
        for c in range(width, PIECES):
            xcopy(1, me, c).start()

    @pl.when(has_right)
    def _():
        send_rest()

    @pl.when(has_left)
    def _():
        for c in range(PIECES):
            xcopy(0, me, c).start()

    with jax.named_scope("know"):
        for d in range(2, n):

            @pl.when((me >= d - 1) & has_right)
            def _():
                pl.semaphore_signal(know.at[0], inc=1, device_id={"head": me + 1}, device_id_type=MESH)

            @pl.when(me >= d)
            def _():
                pl.semaphore_wait(know.at[0], 1)

        if bits == 2:

            @pl.when(spreads)
            def _():
                pl.semaphore_signal(know.at[2], inc=1, device_id={"batch": near[0]}, device_id_type=MESH)

    def tell_left(d):
        @pl.when((me + d - 1 < n) & has_left)
        def _():
            pl.semaphore_signal(know.at[1], inc=1, device_id={"head": me - 1}, device_id_type=MESH)

    def hear_right(d):
        @pl.when(me + d < n)
        def _():
            pl.semaphore_wait(know.at[1], 1)

    if n > 2:
        tell_left(2)

    def w1copy(j):
        at = pl.ds(pl.multiple_of(chip * slab, slab), slab)
        return pltpu.make_async_remote_copy(
            src_ref=ow_hbm.at[at, pl.ds(pl.multiple_of(j * cols, cols), cols)],
            dst_ref=wout.at[me, at],
            send_sem=sent,
            recv_sem=w1r,
            device_id={"head": j},
            device_id_type=MESH,
        )

    def w2copy(j, peer, sem, rows_sent, begin):
        part = wout.at[j, pl.ds(pl.multiple_of(begin, slab), rows_sent)]
        return pltpu.make_async_remote_copy(
            src_ref=part,
            dst_ref=part,
            send_sem=sent,
            recv_sem=sem,
            device_id={"batch": peer},
            device_id_type=MESH,
        )

    def chip_copies(k, j):
        return [
            w2copy(j, base + 2 * lax.rem(chip + o, chips) + parity, chip_r.at[k], slab, chip * slab)
            for o in range(1, chips)
        ]

    def core_copy(k, j):
        return w2copy(j, core_peer, core_r.at[k], heads_rows, 0)

    def spread_chips():
        if bits == 2:
            pl.semaphore_wait(know.at[2], 1)
        landed(wout.at[: n - 1, :slab], w1r)
        for k, j in enumerate(sources):
            for copy in chip_copies(k, j):
                copy.start()

    def spread_cores():
        for k, j in enumerate(sources):
            landed(wout.at[j, : (chips - 1) * slab], chip_r.at[k])
            core_copy(k, j).start()

    def project(j, begin, count, first):
        x = xg[j, pl.ds(begin, count)].reshape(count * seqs, feats)
        at = pl.ds(pl.multiple_of(j * feats, feats), feats)
        part = jnp.dot(x, w[at, :], preferred_element_type=F32)
        gpart = jnp.broadcast_to(rowsum(x.astype(F32) * gate[:, at].astype(F32)), (count * seqs, size))
        at = pl.ds(pl.multiple_of(begin * seqs, seqs), count * seqs)
        if first:
            pacc[at, :] = part
            gacc[at, :] = gpart
        else:
            pacc[at, :] += part
            gacc[at, :] += gpart

    def prepare(start, stop):
        for s in range(start, stop):
            ah, al = split(a32[s])
            mh, ml = split(m32[s])
            bt = lax.dot_general(
                jnp.concatenate([ah, al], axis=1),
                jnp.concatenate([mh, mh], axis=1),
                NT,
                preferred_element_type=F32,
            )
            bt = bt + lax.dot_general(ah, ml, NT, preferred_element_type=F32)
            bh, bl = split(bt)
            ab[s, :size, :size] = ah
            ab[s, size:, :size] = al
            ab[s, :size, size:] = bh
            ab[s, size:, size:] = bl

    for j in sources:

        @pl.when(spreads & (j < me))
        def _():
            w1copy(j).start()

    with jax.named_scope("proj0"):
        for load in loads[1:]:
            load.wait()
        project(me, 0, steps, True)
    with jax.named_scope("prepA"):
        prepare(0, seqs)

    def collect(begin, end):
        for k in range(begin, end):
            j, g = slot_block[k], slot_group[k]
            far = has_right & (me - j >= 2)
            held = far & (parity == 1) & (g == groups - 1)
            for at in range(width):
                c = g * width + at
                with jax.named_scope("x%d_%d" % (k, at)):
                    landed(xg.at[j, pl.ds(c * span, span)], xr.at[slot_of(j, me), c])

                @pl.when((j < me) & has_right & jnp.logical_not(held))
                def _():
                    xcopy(1, j, c).start()

                @pl.when((j > me) & has_left)
                def _():
                    xcopy(0, j, c).start()

            @pl.when(far & (parity == 0) & (g == groups - 1))
            def _():
                pl.semaphore_signal(turn, inc=1, device_id={"batch": core_peer}, device_id_type=MESH)

            @pl.when(held)
            def _():
                with jax.named_scope("t%d" % k):
                    pl.semaphore_wait(turn, 1)
                for c in GROUPS[-1]:
                    xcopy(1, j, c).start()

            with jax.named_scope("p%d" % k):
                project(j, g * width * span, width * span, False)

    past = []
    product = [None]

    def outgoing(part, j, sem):
        return pltpu.make_async_remote_copy(
            src_ref=part,
            dst_ref=part,
            send_sem=sent,
            recv_sem=sem,
            device_id={"head": j},
            device_id_type=MESH,
        )

    def rcopies(j, g):
        sem = rr.at[slot_of(me, j)] if g == groups - 1 else early_r.at[g]
        begin, end = g * width * span * seqs, (g + 1) * width * span * seqs
        return [
            outgoing(rbuf.at[me, pl.ds(begin, end - begin)], j, sem),
            outgoing(sqbuf.at[g, me], j, sem),
        ]

    def send_readouts(g):
        for j in reversed(sources):
            for copy in rcopies(j, g):
                copy.start()

    def advance(g):
        first, last = GROUPS[g][0] * span, (GROUPS[g][-1] + 1) * span
        count = last - first
        half = count * seqs
        at = slice(first * seqs, last * seqs)
        p = pacc[at, :]
        f = 0.8 + 0.2 * jax.nn.sigmoid(gacc[at, :] + bias_ref[...])
        q = p[:, :size]
        k = p[:, size : 2 * size]
        v = p[:, 2 * size :]
        k = k * lax.rsqrt(rowsum(k * k) + 1e-06)
        q = q * lax.rsqrt(rowsum(q * q) + 1e-06)
        kq[:half, :] = k
        kq[half : 2 * half, :] = q
        for s in range(seqs):
            at = pl.ds(s, 2 * count, stride=seqs)
            hi, lo = split(kq[at, :])
            left = jnp.concatenate([hi.astype(F32), lo.astype(F32)], axis=0).astype(BF16)
            r = jnp.dot(jnp.concatenate([left, left], axis=1), ab[s], preferred_element_type=F32)
            r = r[: 2 * count] + r[2 * count :]
            abuf[at, :] = r[:, :size]
            bbuf[at, :] = r[:, size:]

        def piece(x, t):
            return x[t * seqs : (t + 1) * seqs]

        kt = [piece(k, t) for t in range(count)]
        qt = [piece(q, t) for t in range(count)]
        a = [u for u, _, _, _ in past] + [piece(abuf, t) for t in range(count)]
        dots = [[rowsum(a[s] * kt[t]) for s in range(first + t + 1)] for t in range(count)]
        reads = [[rowsum(a[s] * qt[t]) for s in range(first + t + 1)] for t in range(count)]
        pieces = []
        for t in range(count):
            ft = piece(f, t)
            product[0] = ft if product[0] is None else product[0] * ft
            now = first + t
            for s in range(now + 1):
                lower = past[s][1] if s < now else [past[r][2] * dots[t][r] for r in range(now)]
                for r in range(s):
                    dots[t][s] = dots[t][s] - lower[r] * dots[t][r]
                    reads[t][s] = reads[t][s] - lower[r] * reads[t][r]
            weight = 1.0 / (product[0] + dots[t][now])
            value = piece(v, t) - piece(bbuf, t)
            for s in range(now):
                value = value - dots[t][s] * past[s][3]
            past.append((a[now], [past[r][2] * dots[t][r] for r in range(now)], weight, weight * value))
            total = piece(bbuf, count + t)
            for s in range(now + 1):
                total = total + reads[t][s] * past[s][3]
            pieces.append(total)
        ro = jnp.concatenate(pieces, axis=0)
        hi, lo = split(ro * ro)
        both = jnp.concatenate([hi, lo], axis=1)
        sqbuf[g, me] = lax.dot_general(
            jnp.ones((8, 2 * size), BF16),
            jnp.concatenate([both] * (rows // half), axis=0),
            NT,
            preferred_element_type=F32,
        )[:1]
        rbuf[me, first * seqs : last * seqs] = (gain_ref[...] * ro).astype(BF16)

        if g < groups - 1:

            @pl.when(jnp.logical_not(inner))
            def _():
                send_readouts(g)

        else:
            send_readouts(g)

            @pl.when(inner)
            def _():
                for before in range(g):
                    send_readouts(before)

    inner = has_left & has_right
    collect(0, 1)
    if n > 2:
        hear_right(2)
        if n > 3:
            tell_left(3)
    collect(1, 2)
    with jax.named_scope("learn"):
        for d in range(3, n):
            hear_right(d)
            if d + 1 < n:
                tell_left(d + 1)

    collect(2, early - 2)
    for j in sources:

        @pl.when(spreads & (me == 0) & (j < n - 1))
        def _():
            w1copy(j).start()

    collect(early - 2, early - 1)

    @pl.when(spreads & (me == 0))
    def _():
        w1copy(n - 1).start()
        with jax.named_scope("spreadA0"):
            spread_chips()

    collect(early - 1, early)

    @pl.when(inner)
    def _():
        collect(early, len(slot_block))

    for j in sources:

        @pl.when(spreads & inner & (j > me) & (j < n - 1))
        def _():
            w1copy(j).start()

    with jax.named_scope("adv0"):
        advance(0)

    @pl.when(spreads & inner)
    def _():
        w1copy(n - 1).start()

    @pl.when(jnp.logical_not(inner))
    def _():
        collect(early, len(slot_block))

    with jax.named_scope("spreadA1"):

        @pl.when(spreads & (me == n - 1))
        def _():
            spread_chips()

    with jax.named_scope("adv1"):
        advance(1)

    with jax.named_scope("spreadA"):

        @pl.when(spreads & inner)
        def _():
            spread_chips()

    with jax.named_scope("spreadB"):

        @pl.when(spreads)
        def _():
            spread_cores()

    def send_done(part):
        pltpu.make_async_remote_copy(
            src_ref=part,
            dst_ref=part,
            send_sem=sent,
            recv_sem=w1r,
            device_id={"head": me},
            device_id_type=MESH,
        ).wait_send()

    def finish(g):
        part = slice(g * width * span * seqs, (g + 1) * width * span * seqs)
        count = width * span * seqs
        acc = jnp.dot(rbuf[me, part], wout[me], preferred_element_type=F32)
        squares = sqbuf[g, me]
        extra = rows * 4 // (size * 2)
        if g < groups - 1:
            landed(rbuf.at[: n - 1, : count + extra], early_r.at[g])
        for k, j in enumerate(sources):
            if g == 0:

                @pl.when(jnp.logical_not(spreads))
                def _():
                    with jax.named_scope("w%d" % k):
                        landed(wout.at[j], core_r.at[k])

            if g == groups - 1:
                with jax.named_scope("r%d" % k):
                    landed(rbuf.at[j, : count + extra], rr.at[slot_of(j, me)])
            acc = acc + jnp.dot(rbuf[j, part], wout[j], preferred_element_type=F32)
            squares = squares + sqbuf[g, j]
        scale = lax.rsqrt(squares / (n * size) + 1e-06)
        scale = jnp.broadcast_to(scale, (size, rows)).T[:count]
        for at in range(0, cols, size):
            out_ref[part, at : at + size] = acc[:, at : at + size] * scale

    for g in range(groups):
        if g == groups - 1:
            with jax.named_scope("sends"):
                @pl.when(has_right)
                def _():
                    send_done(xg.at[0])

                @pl.when(has_left)
                def _():
                    send_done(xg.at[0])

                for j in sources:

                    @pl.when(inner)
                    def _():
                        send_done(xg.at[0])

                for j in sources:
                    for copy in rcopies(j, 0):
                        copy.wait_send()

        with jax.named_scope("finish%d" % g):
            finish(g)

    @pl.when(spreads)
    def _():
        for _ in sources:
            send_done(wout.at[0, :slab])
            send_done(wout.at[0, : (chips - 1) * slab])
            send_done(wout.at[0])

    for j in sources:
        for copy in rcopies(j, groups - 1):
            copy.wait_send()


def local(n, batch, inputs, in_weight, gate_weight, gate_bias, norm_gain, out_weight, inv_gram, value_key):
    steps, seqs, feats = inputs.shape
    d_model, heads, width = in_weight.shape
    size = width // 3
    rows = steps * seqs
    cols = out_weight.shape[1] // n
    group = math.gcd(math.gcd(batch, 8), out_weight.shape[0] // 16)
    assert heads == 1 and steps % PIECES == 0 and group > 1
    anywhere = pl.BlockSpec(memory_space=pl.ANY)
    vmem = pl.BlockSpec(memory_space=pltpu.VMEM)
    dma = pltpu.SemaphoreType.DMA
    out = pl.pallas_call(
        functools.partial(kernel, n, group),
        out_shape=pltpu.VMEM((rows, cols), F32),
        in_specs=[anywhere] * 8,
        out_specs=vmem,
        scratch_shapes=[
            pltpu.VMEM((1, 1), F32),
            pltpu.VMEM((1, size), F32),
            pltpu.VMEM((n, steps, seqs, feats), BF16),
            pltpu.VMEM((d_model, width), BF16),
            pltpu.VMEM((1, d_model), BF16),
            pltpu.VMEM((seqs, size, size), F32),
            pltpu.VMEM((seqs, size, size), F32),
            pltpu.VMEM((seqs, 2 * size, 2 * size), BF16),
            pltpu.VMEM((n, out_weight.shape[0], cols), BF16),
            pltpu.VMEM((rows, width), F32),
            pltpu.VMEM((rows, size), F32),
            pltpu.VMEM((2 * rows, size), F32),
            pltpu.VMEM((2 * rows, size), F32),
            pltpu.VMEM((2 * rows, size), F32),
            pltpu.VMEM((n, rows, size), BF16),
            pltpu.VMEM((len(GROUPS), n, 1, rows), F32),
            dma((2,)),
            dma((n - 1, PIECES)),
            pltpu.SemaphoreType.REGULAR((3,)),
            pltpu.SemaphoreType.REGULAR,
            dma,
            dma((n - 1,)),
            dma((n - 1,)),
            dma((len(GROUPS) - 1,)),
            dma((n - 1,)),
            dma,
        ],
        compiler_params=pltpu.CompilerParams(collective_id=0, has_side_effects=True),
    )(
        inputs,
        in_weight.reshape(d_model, width),
        gate_weight.reshape(1, d_model),
        gate_bias.reshape(1, 1),
        norm_gain.reshape(1, size),
        out_weight,
        inv_gram.reshape(seqs, size, size),
        value_key.reshape(seqs, size, size),
    )
    return out.reshape(steps, seqs, cols)


def solution(mesh):
    in_specs = (
        P(None, "batch", "head"),
        P(None, "head", None),
        P(None, "head"),
        P("head"),
        P("head"),
        P("head", None),
        P("batch", "head", None, None),
        P("batch", "head", None, None),
    )
    out_specs = P(None, "batch", "head")
    return jax.shard_map(
        functools.partial(local, mesh.shape["head"], mesh.shape["batch"]),
        mesh=mesh,
        in_specs=in_specs,
        out_specs=out_specs,
        check_vma=False,
    )
```

```python
import functools
import math

import jax
import jax.numpy as jnp
from jax import lax
from jax.experimental import pallas as pl
from jax.experimental.pallas import tpu as pltpu
from jax.sharding import PartitionSpec as P

MESH = pl.DeviceIdType.MESH
F32 = jnp.float32
BF16 = jnp.bfloat16
NT = (((1,), (1,)), ((), ()))
PIECES = 4
GROUPS = ((0, 1), (2, 3))


def split(x):
    hi = x.astype(BF16)
    lo = (x - hi.astype(F32)).astype(BF16)
    return hi, lo


def rowsum(x):
    return jnp.sum(x, axis=-1, keepdims=True)


def select(me, values):
    out = jnp.int32(values[0])
    for m in range(1, len(values)):
        out = jnp.where(me == m, jnp.int32(values[m]), out)
    return out


def arrivals(n, groups, width):
    out = []
    for m in range(n):
        found = []
        for j in range(n):
            for g in range(groups):
                hops = abs(j - m)
                late = 0.0 if j < m else 1.7 if j == n - 1 and hops == 1 else 3.0
                found.append(((hops - 1) * groups * width + (g + 1) * width + 2.4 * hops + late, j, g))
        out.append([(j, g) for _, j, g in sorted(found) if j != m])
    return out


def kernel(
    n,
    group,
    x_hbm,
    w_hbm,
    gate_hbm,
    bias_hbm,
    gain_hbm,
    ow_hbm,
    a_hbm,
    m_hbm,
    out_ref,
    bias_ref,
    gain_ref,
    xg,
    w,
    gate,
    a32,
    m32,
    ab,
    wout,
    pacc,
    gacc,
    kq,
    abuf,
    bbuf,
    rbuf,
    sqbuf,
    lsem,
    xr,
    know,
    turn,
    w1r,
    chip_r,
    core_r,
    early_r,
    rr,
    sent,
):
    steps, seqs, feats = x_hbm.shape
    rows = steps * seqs
    heads_rows = ow_hbm.shape[0]
    cols = ow_hbm.shape[1] // n
    size = a_hbm.shape[1]
    me = lax.axis_index("head")
    b = lax.axis_index("batch")
    mine = lax.rem(b, group)
    base = b - mine
    has_left = me > 0
    has_right = me < n - 1

    parity = lax.rem(mine, 2)
    chip = lax.div(mine, 2)
    chips = group // 2
    bits = chips.bit_length() - 1

    def flip(value, bit):
        return value + (1 - 2 * lax.rem(lax.div(value, 1 << bit), 2)) * (1 << bit)

    core_peer = base + mine + 1 - 2 * parity
    near = [base + 2 * flip(chip, bit) + parity for bit in range(bits)]
    slab = heads_rows // chips
    spreads = parity == 1

    barrier = pltpu.get_barrier_semaphore()

    @pl.when(has_left)
    def _():
        pl.semaphore_signal(barrier, inc=1, device_id={"head": me - 1}, device_id_type=MESH)

    @pl.when(has_right)
    def _():
        pl.semaphore_signal(barrier, inc=1, device_id={"head": me + 1}, device_id_type=MESH)

    pl.semaphore_signal(barrier, inc=1, device_id={"batch": core_peer}, device_id_type=MESH)

    @pl.when(spreads)
    def _():
        for peer in near:
            pl.semaphore_signal(barrier, inc=1, device_id={"batch": peer}, device_id_type=MESH)

    loads = [
        pltpu.make_async_copy(x_hbm, xg.at[me], lsem.at[0]),
        pltpu.make_async_copy(w_hbm, w, lsem.at[1]),
        pltpu.make_async_copy(gate_hbm, gate, lsem.at[1]),
        pltpu.make_async_copy(a_hbm, a32, lsem.at[1]),
        pltpu.make_async_copy(m_hbm, m32, lsem.at[1]),
        pltpu.make_async_copy(
            ow_hbm.at[:, pl.ds(pl.multiple_of(me * cols, cols), cols)], wout.at[me], lsem.at[1]
        ),
        pltpu.make_async_copy(bias_hbm, bias_ref, lsem.at[1]),
        pltpu.make_async_copy(gain_hbm, gain_ref, lsem.at[1]),
    ]
    for load in loads:
        load.start()

    order = [sorted((j for j in range(n) if j != m), key=lambda j: (abs(j - m), j)) for m in range(n)]
    sources = [select(me, [order[m][k] for m in range(n)]) for k in range(n - 1)]
    span = steps // PIECES

    groups = len(GROUPS)
    width = len(GROUPS[0])
    slots = arrivals(n, groups, width)
    slot_block = [select(me, [slots[m][k][0] for m in range(n)]) for k in range(len(slots[0]))]
    slot_group = [select(me, [slots[m][k][1] for m in range(n)]) for k in range(len(slots[0]))]
    early = max(k + 1 for m in range(n) for k, (_, g) in enumerate(slots[m]) if g == 0)

    def slot_of(j, receiver):
        return j - (j > receiver).astype(jnp.int32)

    def xcopy(side, j, c):
        part = xg.at[j, pl.ds(c * span, span)]
        peer = me + 2 * side - 1
        return pltpu.make_async_remote_copy(
            src_ref=part,
            dst_ref=part,
            send_sem=sent,
            recv_sem=xr.at[slot_of(j, peer), c],
            device_id={"head": peer},
            device_id_type=MESH,
        )

    def landed(part, sem):
        pltpu.make_async_remote_copy(
            src_ref=part,
            dst_ref=part,
            send_sem=sent,
            recv_sem=sem,
            device_id={"head": me},
            device_id_type=MESH,
        ).wait_recv()

    loads[0].wait()
    with jax.named_scope("barrier"):
        pl.semaphore_wait(barrier, has_left.astype(jnp.int32) + has_right.astype(jnp.int32) + 1 + bits * parity)

    @pl.when(has_right)
    def _():
        for c in GROUPS[0]:
            xcopy(1, me, c).start()

    def send_rest():
        for c in range(width, PIECES):
            xcopy(1, me, c).start()

    @pl.when(has_right)
    def _():
        send_rest()

    @pl.when(has_left)
    def _():
        for c in range(PIECES):
            xcopy(0, me, c).start()

    with jax.named_scope("know"):
        for d in range(2, n):

            @pl.when((me >= d - 1) & has_right)
            def _():
                pl.semaphore_signal(know.at[0], inc=1, device_id={"head": me + 1}, device_id_type=MESH)

            @pl.when(me >= d)
            def _():
                pl.semaphore_wait(know.at[0], 1)

        if bits == 2:

            @pl.when(spreads)
            def _():
                pl.semaphore_signal(know.at[2], inc=1, device_id={"batch": near[0]}, device_id_type=MESH)

    def tell_left(d):
        @pl.when((me + d - 1 < n) & has_left)
        def _():
            pl.semaphore_signal(know.at[1], inc=1, device_id={"head": me - 1}, device_id_type=MESH)

    def hear_right(d):
        @pl.when(me + d < n)
        def _():
            pl.semaphore_wait(know.at[1], 1)

    if n > 2:
        tell_left(2)

    def w1copy(j):
        at = pl.ds(pl.multiple_of(chip * slab, slab), slab)
        return pltpu.make_async_remote_copy(
            src_ref=ow_hbm.at[at, pl.ds(pl.multiple_of(j * cols, cols), cols)],
            dst_ref=wout.at[me, at],
            send_sem=sent,
            recv_sem=w1r,
            device_id={"head": j},
            device_id_type=MESH,
        )

    def w2copy(j, peer, sem, rows_sent, begin):
        part = wout.at[j, pl.ds(pl.multiple_of(begin, slab), rows_sent)]
        return pltpu.make_async_remote_copy(
            src_ref=part,
            dst_ref=part,
            send_sem=sent,
            recv_sem=sem,
            device_id={"batch": peer},
            device_id_type=MESH,
        )

    def chip_copies(k, j):
        return [
            w2copy(j, base + 2 * lax.rem(chip + o, chips) + parity, chip_r.at[k], slab, chip * slab)
            for o in range(1, chips)
        ]

    def core_copy(k, j):
        return w2copy(j, core_peer, core_r.at[k], heads_rows, 0)

    def spread_chips():
        if bits == 2:
            pl.semaphore_wait(know.at[2], 1)
        landed(wout.at[: n - 1, :slab], w1r)
        for k, j in enumerate(sources):
            for copy in chip_copies(k, j):
                copy.start()

    def spread_cores():
        for k, j in enumerate(sources):
            landed(wout.at[j, : (chips - 1) * slab], chip_r.at[k])
            core_copy(k, j).start()

    def project(j, begin, count, first):
        x = xg[j, pl.ds(begin, count)].reshape(count * seqs, feats)
        at = pl.ds(pl.multiple_of(j * feats, feats), feats)
        part = jnp.dot(x, w[at, :], preferred_element_type=F32)
        gpart = jnp.broadcast_to(rowsum(x.astype(F32) * gate[:, at].astype(F32)), (count * seqs, size))
        at = pl.ds(pl.multiple_of(begin * seqs, seqs), count * seqs)
        if first:
            pacc[at, :] = part
            gacc[at, :] = gpart
        else:
            pacc[at, :] += part
            gacc[at, :] += gpart

    def prepare(start, stop):
        for s in range(start, stop):
            ah, al = split(a32[s])
            mh, ml = split(m32[s])
            bt = lax.dot_general(
                jnp.concatenate([ah, al], axis=1),
                jnp.concatenate([mh, mh], axis=1),
                NT,
                preferred_element_type=F32,
            )
            bt = bt + lax.dot_general(ah, ml, NT, preferred_element_type=F32)
            bh, bl = split(bt)
            ab[s, :size, :size] = ah
            ab[s, size:, :size] = al
            ab[s, :size, size:] = bh
            ab[s, size:, size:] = bl

    for j in sources:

        @pl.when(spreads & (j < me))
        def _():
            w1copy(j).start()

    with jax.named_scope("proj0"):
        for load in loads[1:]:
            load.wait()
        project(me, 0, steps, True)
    with jax.named_scope("prepA"):
        prepare(0, seqs)

    def collect(begin, end):
        for k in range(begin, end):
            j, g = slot_block[k], slot_group[k]
            far = has_right & (me - j >= 2)
            held = far & (parity == 1) & (g == groups - 1)
            for at in range(width):
                c = g * width + at
                with jax.named_scope("x%d_%d" % (k, at)):
                    landed(xg.at[j, pl.ds(c * span, span)], xr.at[slot_of(j, me), c])

                @pl.when((j < me) & has_right & jnp.logical_not(held))
                def _():
                    xcopy(1, j, c).start()

                @pl.when((j > me) & has_left)
                def _():
                    xcopy(0, j, c).start()

            @pl.when(held)
            def _():
                with jax.named_scope("t%d" % k):
                    pl.semaphore_wait(turn, 1)
                for c in GROUPS[-1]:
                    xcopy(1, j, c).start()

            with jax.named_scope("p%d" % k):
                project(j, g * width * span, width * span, False)

            @pl.when(far & (parity == 0) & (g == groups - 1))
            def _():
                pl.semaphore_signal(turn, inc=1, device_id={"batch": core_peer}, device_id_type=MESH)

    past = []
    product = [None]

    def outgoing(part, j, sem):
        return pltpu.make_async_remote_copy(
            src_ref=part,
            dst_ref=part,
            send_sem=sent,
            recv_sem=sem,
            device_id={"head": j},
            device_id_type=MESH,
        )

    def rcopies(j, g):
        sem = rr.at[slot_of(me, j)] if g == groups - 1 else early_r.at[g]
        begin, end = g * width * span * seqs, (g + 1) * width * span * seqs
        return [
            outgoing(rbuf.at[me, pl.ds(begin, end - begin)], j, sem),
            outgoing(sqbuf.at[g, me], j, sem),
        ]

    def send_readouts(g):
        for j in reversed(sources):
            for copy in rcopies(j, g):
                copy.start()

    def advance(g):
        first, last = GROUPS[g][0] * span, (GROUPS[g][-1] + 1) * span
        count = last - first
        half = count * seqs
        at = slice(first * seqs, last * seqs)
        p = pacc[at, :]
        f = 0.8 + 0.2 * jax.nn.sigmoid(gacc[at, :] + bias_ref[...])
        q = p[:, :size]
        k = p[:, size : 2 * size]
        v = p[:, 2 * size :]
        kq[:half, :] = k
        kq[half : 2 * half, :] = q
        for s in range(seqs):
            at = pl.ds(s, 2 * count, stride=seqs)
            hi, lo = split(kq[at, :])
            left = jnp.concatenate([hi.astype(F32), lo.astype(F32)], axis=0).astype(BF16)
            r = jnp.dot(jnp.concatenate([left, left], axis=1), ab[s], preferred_element_type=F32)
            r = r[: 2 * count] + r[2 * count :]
            abuf[at, :] = r[:, :size]
            bbuf[at, :] = r[:, size:]

        def piece(x, t):
            return x[t * seqs : (t + 1) * seqs]

        over_k = lax.rsqrt(rowsum(k * k) + 1e-06)
        over_q = lax.rsqrt(rowsum(q * q) + 1e-06)
        k = k * over_k
        q = q * over_q
        ak = abuf[:half, :] * over_k
        bk = bbuf[:half, :] * over_k
        bq = bbuf[half : 2 * half, :] * over_q
        kt = [piece(k, t) for t in range(count)]
        qt = [piece(q, t) for t in range(count)]
        a = [u for u, _, _, _ in past] + [piece(ak, t) for t in range(count)]
        dots = [[rowsum(a[s] * kt[t]) for s in range(first + t + 1)] for t in range(count)]
        reads = [[rowsum(a[s] * qt[t]) for s in range(first + t + 1)] for t in range(count)]
        pieces = []
        for t in range(count):
            ft = piece(f, t)
            product[0] = ft if product[0] is None else product[0] * ft
            now = first + t
            for s in range(now + 1):
                lower = past[s][1] if s < now else [past[r][2] * dots[t][r] for r in range(now)]
                for r in range(s):
                    dots[t][s] = dots[t][s] - lower[r] * dots[t][r]
                    reads[t][s] = reads[t][s] - lower[r] * reads[t][r]
            weight = 1.0 / (product[0] + dots[t][now])
            value = piece(v, t) - piece(bk, t)
            for s in range(now):
                value = value - dots[t][s] * past[s][3]
            past.append((a[now], [past[r][2] * dots[t][r] for r in range(now)], weight, weight * value))
            total = piece(bq, t)
            for s in range(now + 1):
                total = total + reads[t][s] * past[s][3]
            pieces.append(total)
        ro = jnp.concatenate(pieces, axis=0)
        hi, lo = split(ro * ro)
        both = jnp.concatenate([hi, lo], axis=1)
        sqbuf[g, me] = lax.dot_general(
            jnp.ones((8, 2 * size), BF16),
            jnp.concatenate([both] * (rows // half), axis=0),
            NT,
            preferred_element_type=F32,
        )[:1]
        rbuf[me, first * seqs : last * seqs] = (gain_ref[...] * ro).astype(BF16)

        if g < groups - 1:

            @pl.when(jnp.logical_not(inner))
            def _():
                send_readouts(g)

        else:
            send_readouts(g)

            @pl.when(inner)
            def _():
                for before in range(g):
                    send_readouts(before)

    inner = has_left & has_right
    collect(0, 1)
    if n > 2:
        hear_right(2)
        if n > 3:
            tell_left(3)
    collect(1, 2)
    with jax.named_scope("learn"):
        for d in range(3, n):
            hear_right(d)
            if d + 1 < n:
                tell_left(d + 1)

    collect(2, early - 2)
    for j in sources:

        @pl.when(spreads & (me == 0) & (j < n - 1))
        def _():
            w1copy(j).start()

    collect(early - 2, early - 1)

    @pl.when(spreads & (me == 0))
    def _():
        w1copy(n - 1).start()
        with jax.named_scope("spreadA0"):
            spread_chips()

    collect(early - 1, early)

    @pl.when(inner)
    def _():
        collect(early, len(slot_block))

    for j in sources:

        @pl.when(spreads & inner & (j > me) & (j < n - 1))
        def _():
            w1copy(j).start()

    with jax.named_scope("adv0"):
        advance(0)

    @pl.when(spreads & inner)
    def _():
        w1copy(n - 1).start()

    @pl.when(jnp.logical_not(inner))
    def _():
        collect(early, len(slot_block))

    with jax.named_scope("adv1"):
        advance(1)

    with jax.named_scope("spreadA"):

        @pl.when(spreads & (me > 0))
        def _():
            spread_chips()

    with jax.named_scope("spreadB"):

        @pl.when(spreads)
        def _():
            spread_cores()

    def send_done(part):
        pltpu.make_async_remote_copy(
            src_ref=part,
            dst_ref=part,
            send_sem=sent,
            recv_sem=w1r,
            device_id={"head": me},
            device_id_type=MESH,
        ).wait_send()

    def finish(g):
        part = slice(g * width * span * seqs, (g + 1) * width * span * seqs)
        count = width * span * seqs
        acc = jnp.dot(rbuf[me, part], wout[me], preferred_element_type=F32)
        squares = sqbuf[g, me]
        extra = rows * 4 // (size * 2)
        if g < groups - 1:
            landed(rbuf.at[: n - 1, : count + extra], early_r.at[g])
        for k, j in enumerate(sources):
            if g == 0:

                @pl.when(jnp.logical_not(spreads))
                def _():
                    with jax.named_scope("w%d" % k):
                        landed(wout.at[j], core_r.at[k])

            if g == groups - 1:
                with jax.named_scope("r%d" % k):
                    landed(rbuf.at[j, : count + extra], rr.at[slot_of(j, me)])
            acc = acc + jnp.dot(rbuf[j, part], wout[j], preferred_element_type=F32)
            squares = squares + sqbuf[g, j]
        scale = lax.rsqrt(squares / (n * size) + 1e-06)
        scale = jnp.broadcast_to(scale, (size, rows)).T[:count]
        for at in range(0, cols, size):
            out_ref[part, at : at + size] = acc[:, at : at + size] * scale

    for g in range(groups):
        if g == groups - 1:
            with jax.named_scope("sends"):
                @pl.when(has_right)
                def _():
                    send_done(xg.at[0])

                @pl.when(has_left)
                def _():
                    send_done(xg.at[0])

                for j in sources:

                    @pl.when(inner)
                    def _():
                        send_done(xg.at[0])

                for j in sources:
                    for copy in rcopies(j, 0):
                        copy.wait_send()

        with jax.named_scope("finish%d" % g):
            finish(g)

    @pl.when(spreads)
    def _():
        for _ in sources:
            send_done(wout.at[0, :slab])
            send_done(wout.at[0, : (chips - 1) * slab])
            send_done(wout.at[0])

    for j in sources:
        for copy in rcopies(j, groups - 1):
            copy.wait_send()


def local(n, batch, inputs, in_weight, gate_weight, gate_bias, norm_gain, out_weight, inv_gram, value_key):
    steps, seqs, feats = inputs.shape
    d_model, heads, width = in_weight.shape
    size = width // 3
    rows = steps * seqs
    cols = out_weight.shape[1] // n
    group = math.gcd(math.gcd(batch, 8), out_weight.shape[0] // 16)
    assert heads == 1 and steps % PIECES == 0 and group > 1
    anywhere = pl.BlockSpec(memory_space=pl.ANY)
    vmem = pl.BlockSpec(memory_space=pltpu.VMEM)
    dma = pltpu.SemaphoreType.DMA
    out = pl.pallas_call(
        functools.partial(kernel, n, group),
        out_shape=pltpu.VMEM((rows, cols), F32),
        in_specs=[anywhere] * 8,
        out_specs=vmem,
        scratch_shapes=[
            pltpu.VMEM((1, 1), F32),
            pltpu.VMEM((1, size), F32),
            pltpu.VMEM((n, steps, seqs, feats), BF16),
            pltpu.VMEM((d_model, width), BF16),
            pltpu.VMEM((1, d_model), BF16),
            pltpu.VMEM((seqs, size, size), F32),
            pltpu.VMEM((seqs, size, size), F32),
            pltpu.VMEM((seqs, 2 * size, 2 * size), BF16),
            pltpu.VMEM((n, out_weight.shape[0], cols), BF16),
            pltpu.VMEM((rows, width), F32),
            pltpu.VMEM((rows, size), F32),
            pltpu.VMEM((2 * rows, size), F32),
            pltpu.VMEM((2 * rows, size), F32),
            pltpu.VMEM((2 * rows, size), F32),
            pltpu.VMEM((n, rows, size), BF16),
            pltpu.VMEM((len(GROUPS), n, 1, rows), F32),
            dma((2,)),
            dma((n - 1, PIECES)),
            pltpu.SemaphoreType.REGULAR((3,)),
            pltpu.SemaphoreType.REGULAR,
            dma,
            dma((n - 1,)),
            dma((n - 1,)),
            dma((len(GROUPS) - 1,)),
            dma((n - 1,)),
            dma,
        ],
        compiler_params=pltpu.CompilerParams(collective_id=0, has_side_effects=True),
    )(
        inputs,
        in_weight.reshape(d_model, width),
        gate_weight.reshape(1, d_model),
        gate_bias.reshape(1, 1),
        norm_gain.reshape(1, size),
        out_weight,
        inv_gram.reshape(seqs, size, size),
        value_key.reshape(seqs, size, size),
    )
    return out.reshape(steps, seqs, cols)


def solution(mesh):
    in_specs = (
        P(None, "batch", "head"),
        P(None, "head", None),
        P(None, "head"),
        P("head"),
        P("head"),
        P("head", None),
        P("batch", "head", None, None),
        P("batch", "head", None, None),
    )
    out_specs = P(None, "batch", "head")
    return jax.shard_map(
        functools.partial(local, mesh.shape["head"], mesh.shape["batch"]),
        mesh=mesh,
        in_specs=in_specs,
        out_specs=out_specs,
        check_vma=False,
    )
```

```python
import functools
import math

import jax
import jax.numpy as jnp
from jax import lax
from jax.experimental import pallas as pl
from jax.experimental.pallas import tpu as pltpu
from jax.sharding import PartitionSpec as P

MESH = pl.DeviceIdType.MESH
F32 = jnp.float32
BF16 = jnp.bfloat16
NT = (((1,), (1,)), ((), ()))
PIECES = 4
GROUPS = ((0, 1), (2, 3))


def split(x):
    hi = x.astype(BF16)
    lo = (x - hi.astype(F32)).astype(BF16)
    return hi, lo


def rowsum(x):
    return jnp.sum(x, axis=-1, keepdims=True)


def select(me, values):
    out = jnp.int32(values[0])
    for m in range(1, len(values)):
        out = jnp.where(me == m, jnp.int32(values[m]), out)
    return out


def arrivals(n, groups, width):
    out = []
    for m in range(n):
        found = []
        for j in range(n):
            for g in range(groups):
                hops = abs(j - m)
                late = 0.0 if j < m else 1.7 if j == n - 1 and hops == 1 else 3.0
                found.append(((hops - 1) * groups * width + (g + 1) * width + 2.4 * hops + late, j, g))
        out.append([(j, g) for _, j, g in sorted(found) if j != m])
    return out


def kernel(
    n,
    group,
    x_hbm,
    w_hbm,
    gate_hbm,
    bias_hbm,
    gain_hbm,
    ow_hbm,
    a_hbm,
    m_hbm,
    out_ref,
    bias_ref,
    gain_ref,
    xg,
    w,
    gate,
    a32,
    m32,
    ab,
    wout,
    pacc,
    gacc,
    kq,
    abuf,
    bbuf,
    rbuf,
    sqbuf,
    lsem,
    xr,
    know,
    turn,
    w1r,
    chip_r,
    early_r,
    rr,
    sent,
):
    steps, seqs, feats = x_hbm.shape
    rows = steps * seqs
    heads_rows = ow_hbm.shape[0]
    cols = ow_hbm.shape[1] // n
    size = a_hbm.shape[1]
    me = lax.axis_index("head")
    b = lax.axis_index("batch")
    mine = lax.rem(b, group)
    base = b - mine
    has_left = me > 0
    has_right = me < n - 1

    parity = lax.rem(mine, 2)
    chip = lax.div(mine, 2)
    chips = group // 2
    bits = chips.bit_length() - 1

    def flip(value, bit):
        return value + (1 - 2 * lax.rem(lax.div(value, 1 << bit), 2)) * (1 << bit)

    core_peer = base + mine + 1 - 2 * parity
    near = [base + 2 * flip(chip, bit) + parity for bit in range(bits)]
    slab = heads_rows // chips
    spreads = parity == 1

    barrier = pltpu.get_barrier_semaphore()

    @pl.when(has_left)
    def _():
        pl.semaphore_signal(barrier, inc=1, device_id={"head": me - 1}, device_id_type=MESH)

    @pl.when(has_right)
    def _():
        pl.semaphore_signal(barrier, inc=1, device_id={"head": me + 1}, device_id_type=MESH)

    pl.semaphore_signal(barrier, inc=1, device_id={"batch": core_peer}, device_id_type=MESH)

    @pl.when(spreads)
    def _():
        for peer in near:
            pl.semaphore_signal(barrier, inc=1, device_id={"batch": peer}, device_id_type=MESH)

    loads = [
        pltpu.make_async_copy(x_hbm, xg.at[me], lsem.at[0]),
        pltpu.make_async_copy(w_hbm, w, lsem.at[1]),
        pltpu.make_async_copy(gate_hbm, gate, lsem.at[1]),
        pltpu.make_async_copy(a_hbm, a32, lsem.at[1]),
        pltpu.make_async_copy(m_hbm, m32, lsem.at[1]),
        pltpu.make_async_copy(
            ow_hbm.at[:, pl.ds(pl.multiple_of(me * cols, cols), cols)], wout.at[me], lsem.at[1]
        ),
        pltpu.make_async_copy(bias_hbm, bias_ref, lsem.at[1]),
        pltpu.make_async_copy(gain_hbm, gain_ref, lsem.at[1]),
    ]
    loads[0].start()

    order = [sorted((j for j in range(n) if j != m), key=lambda j: (abs(j - m), j)) for m in range(n)]
    sources = [select(me, [order[m][k] for m in range(n)]) for k in range(n - 1)]
    span = steps // PIECES

    groups = len(GROUPS)
    width = len(GROUPS[0])
    slots = arrivals(n, groups, width)
    slot_block = [select(me, [slots[m][k][0] for m in range(n)]) for k in range(len(slots[0]))]
    slot_group = [select(me, [slots[m][k][1] for m in range(n)]) for k in range(len(slots[0]))]
    early = max(k + 1 for m in range(n) for k, (_, g) in enumerate(slots[m]) if g == 0)

    def slot_of(j, receiver):
        return j - (j > receiver).astype(jnp.int32)

    def xcopy(side, j, c):
        part = xg.at[j, pl.ds(c * span, span)]
        peer = me + 2 * side - 1
        return pltpu.make_async_remote_copy(
            src_ref=part,
            dst_ref=part,
            send_sem=sent,
            recv_sem=xr.at[slot_of(j, peer), c],
            device_id={"head": peer},
            device_id_type=MESH,
        )

    def landed(part, sem):
        pltpu.make_async_remote_copy(
            src_ref=part,
            dst_ref=part,
            send_sem=sent,
            recv_sem=sem,
            device_id={"head": me},
            device_id_type=MESH,
        ).wait_recv()

    loads[0].wait()
    for load in loads[1:]:
        load.start()
    with jax.named_scope("barrier"):
        pl.semaphore_wait(barrier, has_left.astype(jnp.int32) + has_right.astype(jnp.int32) + 1 + bits * parity)

    @pl.when(has_right)
    def _():
        for c in GROUPS[0]:
            xcopy(1, me, c).start()

    def send_rest():
        for c in range(width, PIECES):
            xcopy(1, me, c).start()

    @pl.when(has_right)
    def _():
        send_rest()

    @pl.when(has_left)
    def _():
        for c in range(PIECES):
            xcopy(0, me, c).start()

    with jax.named_scope("know"):
        for d in range(2, n):

            @pl.when((me >= d - 1) & has_right)
            def _():
                pl.semaphore_signal(know.at[0], inc=1, device_id={"head": me + 1}, device_id_type=MESH)

            @pl.when(me >= d)
            def _():
                pl.semaphore_wait(know.at[0], 1)

        if bits == 2:

            @pl.when(spreads)
            def _():
                pl.semaphore_signal(know.at[2], inc=1, device_id={"batch": near[0]}, device_id_type=MESH)

    def tell_left(d):
        @pl.when((me + d - 1 < n) & has_left)
        def _():
            pl.semaphore_signal(know.at[1], inc=1, device_id={"head": me - 1}, device_id_type=MESH)

    def hear_right(d):
        @pl.when(me + d < n)
        def _():
            pl.semaphore_wait(know.at[1], 1)

    if n > 2:
        tell_left(2)

    def w1copy(j):
        at = pl.ds(pl.multiple_of(chip * slab, slab), slab)
        return pltpu.make_async_remote_copy(
            src_ref=ow_hbm.at[at, pl.ds(pl.multiple_of(j * cols, cols), cols)],
            dst_ref=wout.at[me, at],
            send_sem=sent,
            recv_sem=w1r,
            device_id={"head": j},
            device_id_type=MESH,
        )

    def w2copy(j, peer, sem, rows_sent, begin):
        part = wout.at[j, pl.ds(pl.multiple_of(begin, slab), rows_sent)]
        return pltpu.make_async_remote_copy(
            src_ref=part,
            dst_ref=part,
            send_sem=sent,
            recv_sem=sem,
            device_id={"batch": peer},
            device_id_type=MESH,
        )

    def chip_copies(k, j):
        return [
            w2copy(j, base + 2 * lax.rem(chip + o, chips) + parity, chip_r.at[k], slab, chip * slab)
            for o in range(1, chips)
        ]

    def core_copy(k, j):
        return w2copy(j, core_peer, chip_r.at[k], heads_rows, 0)

    def spread_chips():
        if bits == 2:
            pl.semaphore_wait(know.at[2], 1)
        landed(wout.at[: n - 1, :slab], w1r)
        copies = [chip_copies(k, j) for k, j in enumerate(sources)]
        for o in range(chips - 1):
            for found in copies:
                found[o].start()

    def spread_cores():
        for k, j in enumerate(sources):
            landed(wout.at[j, : (chips - 1) * slab], chip_r.at[k])
            core_copy(k, j).start()

    def project(j, begin, count, first):
        x = xg[j, pl.ds(begin, count)].reshape(count * seqs, feats)
        at = pl.ds(pl.multiple_of(j * feats, feats), feats)
        part = jnp.dot(x, w[at, :], preferred_element_type=F32)
        gpart = jnp.broadcast_to(rowsum(x.astype(F32) * gate[:, at].astype(F32)), (count * seqs, size))
        at = pl.ds(pl.multiple_of(begin * seqs, seqs), count * seqs)
        if first:
            pacc[at, :] = part
            gacc[at, :] = gpart
        else:
            pacc[at, :] += part
            gacc[at, :] += gpart

    def prepare(start, stop):
        for s in range(start, stop):
            ah, al = split(a32[s])
            mh, ml = split(m32[s])
            bt = lax.dot_general(
                jnp.concatenate([ah, al], axis=1),
                jnp.concatenate([mh, mh], axis=1),
                NT,
                preferred_element_type=F32,
            )
            bt = bt + lax.dot_general(ah, ml, NT, preferred_element_type=F32)
            bh, bl = split(bt)
            ab[s, :size, :size] = ah
            ab[s, size:, :size] = al
            ab[s, :size, size:] = bh
            ab[s, size:, size:] = bl

    for j in sources:

        @pl.when(spreads & (j < me))
        def _():
            w1copy(j).start()

    with jax.named_scope("proj0"):
        for load in loads[1:]:
            load.wait()
        project(me, 0, steps, True)
    with jax.named_scope("prepA"):
        prepare(0, seqs)

    def collect(begin, end):
        for k in range(begin, end):
            j, g = slot_block[k], slot_group[k]
            far = has_right & (me - j >= 2)
            held = far & (parity == 1) & (g == groups - 1)
            for at in range(width):
                c = g * width + at
                with jax.named_scope("x%d_%d" % (k, at)):
                    landed(xg.at[j, pl.ds(c * span, span)], xr.at[slot_of(j, me), c])

                @pl.when((j < me) & has_right & jnp.logical_not(held))
                def _():
                    xcopy(1, j, c).start()

                @pl.when((j > me) & has_left)
                def _():
                    xcopy(0, j, c).start()

            @pl.when(held)
            def _():
                with jax.named_scope("t%d" % k):
                    pl.semaphore_wait(turn, 1)
                for c in GROUPS[-1]:
                    xcopy(1, j, c).start()

            with jax.named_scope("p%d" % k):
                project(j, g * width * span, width * span, False)

    past = []
    product = [None]

    def outgoing(part, j, sem):
        return pltpu.make_async_remote_copy(
            src_ref=part,
            dst_ref=part,
            send_sem=sent,
            recv_sem=sem,
            device_id={"head": j},
            device_id_type=MESH,
        )

    def rcopies(j, g):
        sem = rr.at[slot_of(me, j)] if g == groups - 1 else early_r.at[g]
        begin, end = g * width * span * seqs, (g + 1) * width * span * seqs
        return [
            outgoing(rbuf.at[me, pl.ds(begin, end - begin)], j, sem),
            outgoing(sqbuf.at[g, me], j, sem),
        ]

    def send_readouts(g):
        for k in range(n - 1):
            for copy in rcopies(jnp.where(inner, sources[k], sources[n - 2 - k]), g):
                copy.start()

    def advance(g):
        first, last = GROUPS[g][0] * span, (GROUPS[g][-1] + 1) * span
        count = last - first
        half = count * seqs
        at = slice(first * seqs, last * seqs)
        p = pacc[at, :]
        f = 0.8 + 0.2 * jax.nn.sigmoid(gacc[at, :] + bias_ref[...])
        q = p[:, :size]
        k = p[:, size : 2 * size]
        v = p[:, 2 * size :]
        kq[:half, :] = k
        kq[half : 2 * half, :] = q
        for s in range(seqs):
            at = pl.ds(s, 2 * count, stride=seqs)
            hi, lo = split(kq[at, :])
            left = jnp.concatenate([hi.astype(F32), lo.astype(F32)], axis=0).astype(BF16)
            r = jnp.dot(jnp.concatenate([left, left], axis=1), ab[s], preferred_element_type=F32)
            r = r[: 2 * count] + r[2 * count :]
            abuf[at, :] = r[:, :size]
            bbuf[at, :] = r[:, size:]

        def piece(x, t):
            return x[t * seqs : (t + 1) * seqs]

        over_k = lax.rsqrt(rowsum(k * k) + 1e-06)
        over_q = lax.rsqrt(rowsum(q * q) + 1e-06)
        k = k * over_k
        q = q * over_q
        ak = abuf[:half, :] * over_k
        bk = bbuf[:half, :] * over_k
        bq = bbuf[half : 2 * half, :] * over_q
        kt = [piece(k, t) for t in range(count)]
        qt = [piece(q, t) for t in range(count)]
        a = [u for u, _, _, _ in past] + [piece(ak, t) for t in range(count)]
        dots = [[rowsum(a[s] * kt[t]) for s in range(first + t + 1)] for t in range(count)]
        reads = [[rowsum(a[s] * qt[t]) for s in range(first + t + 1)] for t in range(count)]
        pieces = []
        for t in range(count):
            ft = piece(f, t)
            product[0] = ft if product[0] is None else product[0] * ft
            now = first + t
            for s in range(now + 1):
                lower = past[s][1] if s < now else [past[r][2] * dots[t][r] for r in range(now)]
                for r in range(s):
                    dots[t][s] = dots[t][s] - lower[r] * dots[t][r]
                    reads[t][s] = reads[t][s] - lower[r] * reads[t][r]
            weight = 1.0 / (product[0] + dots[t][now])
            value = piece(v, t) - piece(bk, t)
            for s in range(now):
                value = value - dots[t][s] * past[s][3]
            past.append((a[now], [past[r][2] * dots[t][r] for r in range(now)], weight, weight * value))
            total = piece(bq, t)
            for s in range(now + 1):
                total = total + reads[t][s] * past[s][3]
            pieces.append(total)
        ro = jnp.concatenate(pieces, axis=0)
        hi, lo = split(ro * ro)
        both = jnp.concatenate([hi, lo], axis=1)
        sqbuf[g, me] = lax.dot_general(
            jnp.ones((8, 2 * size), BF16),
            jnp.concatenate([both] * (rows // half), axis=0),
            NT,
            preferred_element_type=F32,
        )[:1]
        rbuf[me, first * seqs : last * seqs] = (gain_ref[...] * ro).astype(BF16)

        if g < groups - 1:

            @pl.when(jnp.logical_not(inner))
            def _():
                send_readouts(g)

        else:
            send_readouts(g)

            @pl.when(inner)
            def _():
                for before in range(g):
                    send_readouts(before)

    inner = has_left & has_right
    collect(0, 1)
    if n > 2:
        hear_right(2)
        if n > 3:
            tell_left(3)
    collect(1, 2)
    with jax.named_scope("learn"):
        for d in range(3, n):
            hear_right(d)
            if d + 1 < n:
                tell_left(d + 1)

    collect(2, early - 2)
    for j in sources:

        @pl.when(spreads & (me == 0) & (j < n - 1))
        def _():
            w1copy(j).start()

    collect(early - 2, early - 1)

    @pl.when(spreads & (me == 0))
    def _():
        with jax.named_scope("spreadA0"):
            spread_chips()
        w1copy(n - 1).start()

    collect(early - 1, early)

    @pl.when(inner)
    def _():
        collect(early, len(slot_block))

    for j in sources:

        @pl.when(spreads & inner & (j > me) & (j < n - 1))
        def _():
            w1copy(j).start()

    with jax.named_scope("adv0"):
        advance(0)

    for k in range(len(slot_block)):

        @pl.when(has_right & (me - slot_block[k] >= 2) & (parity == 0) & (slot_group[k] == groups - 1))
        def _():
            pl.semaphore_signal(turn, inc=1, device_id={"batch": core_peer}, device_id_type=MESH)

    @pl.when(spreads & inner & (me < n - 2))
    def _():
        w1copy(n - 1).start()

    @pl.when(spreads & inner & (me == n - 2))
    def _():
        w1copy(n - 1).start()

    @pl.when(jnp.logical_not(inner))
    def _():
        collect(early, len(slot_block))

    with jax.named_scope("adv1"):
        advance(1)

    with jax.named_scope("spreadA"):

        @pl.when(spreads & (me > 0))
        def _():
            spread_chips()

    with jax.named_scope("spreadB"):

        @pl.when(spreads)
        def _():
            spread_cores()

    def send_done(part):
        pltpu.make_async_remote_copy(
            src_ref=part,
            dst_ref=part,
            send_sem=sent,
            recv_sem=w1r,
            device_id={"head": me},
            device_id_type=MESH,
        ).wait_send()

    def finish(g):
        part = slice(g * width * span * seqs, (g + 1) * width * span * seqs)
        count = width * span * seqs
        acc = jnp.dot(rbuf[me, part], wout[me], preferred_element_type=F32)
        squares = sqbuf[g, me]
        extra = rows * 4 // (size * 2)
        if g < groups - 1:
            landed(rbuf.at[: n - 1, : count + extra], early_r.at[g])
        for k, j in enumerate(sources):
            if g == 0:

                @pl.when(jnp.logical_not(spreads))
                def _():
                    with jax.named_scope("w%d" % k):
                        landed(wout.at[j], chip_r.at[k])

            if g == groups - 1:
                with jax.named_scope("r%d" % k):
                    landed(rbuf.at[j, : count + extra], rr.at[slot_of(j, me)])
            acc = acc + jnp.dot(rbuf[j, part], wout[j], preferred_element_type=F32)
            squares = squares + sqbuf[g, j]
        scale = lax.rsqrt(squares / (n * size) + 1e-06)
        scale = jnp.broadcast_to(scale, (size, rows)).T[:count]
        for at in range(0, cols, size):
            out_ref[part, at : at + size] = acc[:, at : at + size] * scale

    for g in range(groups):
        if g == groups - 1:
            with jax.named_scope("sends"):
                @pl.when(has_right)
                def _():
                    send_done(xg.at[0])

                @pl.when(has_left)
                def _():
                    send_done(xg.at[0])

                for j in sources:

                    @pl.when(inner)
                    def _():
                        send_done(xg.at[0])

                for j in sources:
                    for copy in rcopies(j, 0):
                        copy.wait_send()

        with jax.named_scope("finish%d" % g):
            finish(g)

    @pl.when(spreads)
    def _():
        for _ in sources:
            send_done(wout.at[0, :slab])
            send_done(wout.at[0, : (chips - 1) * slab])
            send_done(wout.at[0])

    for j in sources:
        for copy in rcopies(j, groups - 1):
            copy.wait_send()


def local(n, batch, inputs, in_weight, gate_weight, gate_bias, norm_gain, out_weight, inv_gram, value_key):
    steps, seqs, feats = inputs.shape
    d_model, heads, width = in_weight.shape
    size = width // 3
    rows = steps * seqs
    cols = out_weight.shape[1] // n
    group = math.gcd(math.gcd(batch, 8), out_weight.shape[0] // 16)
    assert heads == 1 and steps % PIECES == 0 and group > 1
    anywhere = pl.BlockSpec(memory_space=pl.ANY)
    vmem = pl.BlockSpec(memory_space=pltpu.VMEM)
    dma = pltpu.SemaphoreType.DMA
    out = pl.pallas_call(
        functools.partial(kernel, n, group),
        out_shape=pltpu.VMEM((rows, cols), F32),
        in_specs=[anywhere] * 8,
        out_specs=vmem,
        scratch_shapes=[
            pltpu.VMEM((1, 1), F32),
            pltpu.VMEM((1, size), F32),
            pltpu.VMEM((n, steps, seqs, feats), BF16),
            pltpu.VMEM((d_model, width), BF16),
            pltpu.VMEM((1, d_model), BF16),
            pltpu.VMEM((seqs, size, size), F32),
            pltpu.VMEM((seqs, size, size), F32),
            pltpu.VMEM((seqs, 2 * size, 2 * size), BF16),
            pltpu.VMEM((n, out_weight.shape[0], cols), BF16),
            pltpu.VMEM((rows, width), F32),
            pltpu.VMEM((rows, size), F32),
            pltpu.VMEM((2 * rows, size), F32),
            pltpu.VMEM((2 * rows, size), F32),
            pltpu.VMEM((2 * rows, size), F32),
            pltpu.VMEM((n, rows, size), BF16),
            pltpu.VMEM((len(GROUPS), n, 1, rows), F32),
            dma((2,)),
            dma((n - 1, PIECES)),
            pltpu.SemaphoreType.REGULAR((3,)),
            pltpu.SemaphoreType.REGULAR,
            dma,
            dma((n - 1,)),
            dma((len(GROUPS) - 1,)),
            dma((n - 1,)),
            dma,
        ],
        compiler_params=pltpu.CompilerParams(collective_id=0, has_side_effects=True),
    )(
        inputs,
        in_weight.reshape(d_model, width),
        gate_weight.reshape(1, d_model),
        gate_bias.reshape(1, 1),
        norm_gain.reshape(1, size),
        out_weight,
        inv_gram.reshape(seqs, size, size),
        value_key.reshape(seqs, size, size),
    )
    return out.reshape(steps, seqs, cols)


def solution(mesh):
    in_specs = (
        P(None, "batch", "head"),
        P(None, "head", None),
        P(None, "head"),
        P("head"),
        P("head"),
        P("head", None),
        P("batch", "head", None, None),
        P("batch", "head", None, None),
    )
    out_specs = P(None, "batch", "head")
    return jax.shard_map(
        functools.partial(local, mesh.shape["head"], mesh.shape["batch"]),
        mesh=mesh,
        in_specs=in_specs,
        out_specs=out_specs,
        check_vma=False,
    )
```

```python
import functools
import math

import jax
import jax.numpy as jnp
from jax import lax
from jax.experimental import pallas as pl
from jax.experimental.pallas import tpu as pltpu
from jax.sharding import PartitionSpec as P

MESH = pl.DeviceIdType.MESH
F32 = jnp.float32
BF16 = jnp.bfloat16
NT = (((1,), (1,)), ((), ()))
PIECES = 4
GROUPS = ((0, 1), (2, 3))


def split(x):
    hi = x.astype(BF16)
    lo = (x - hi.astype(F32)).astype(BF16)
    return hi, lo


def rowsum(x):
    return jnp.sum(x, axis=-1, keepdims=True)


def select(me, values):
    out = jnp.int32(values[0])
    for m in range(1, len(values)):
        out = jnp.where(me == m, jnp.int32(values[m]), out)
    return out


def arrivals(n, groups, width):
    out = []
    for m in range(n):
        found = []
        for j in range(n):
            for g in range(groups):
                hops = abs(j - m)
                late = 0.0 if j < m else 1.7 if j == n - 1 and hops == 1 else 3.0
                found.append(((hops - 1) * groups * width + (g + 1) * width + 2.4 * hops + late, j, g))
        out.append([(j, g) for _, j, g in sorted(found) if j != m])
    return out


def kernel(
    n,
    group,
    x_hbm,
    w_hbm,
    gate_hbm,
    bias_hbm,
    gain_hbm,
    ow_hbm,
    a_hbm,
    m_hbm,
    out_ref,
    bias_ref,
    gain_ref,
    xg,
    w,
    gate,
    a32,
    m32,
    ab,
    wout,
    pacc,
    gacc,
    kq,
    abuf,
    bbuf,
    rbuf,
    sqbuf,
    lsem,
    xr,
    know,
    turn,
    w1r,
    chip_r,
    early_r,
    rr,
    sent,
):
    steps, seqs, feats = x_hbm.shape
    rows = steps * seqs
    heads_rows = ow_hbm.shape[0]
    cols = ow_hbm.shape[1] // n
    size = a_hbm.shape[1]
    me = lax.axis_index("head")
    b = lax.axis_index("batch")
    mine = lax.rem(b, group)
    base = b - mine
    has_left = me > 0
    has_right = me < n - 1

    parity = lax.rem(mine, 2)
    chip = lax.div(mine, 2)
    chips = group // 2
    bits = chips.bit_length() - 1

    def flip(value, bit):
        return value + (1 - 2 * lax.rem(lax.div(value, 1 << bit), 2)) * (1 << bit)

    core_peer = base + mine + 1 - 2 * parity
    near = [base + 2 * flip(chip, bit) + parity for bit in range(bits)]
    slab = heads_rows // chips
    spreads = parity == 1

    barrier = pltpu.get_barrier_semaphore()

    @pl.when(has_left)
    def _():
        pl.semaphore_signal(barrier, inc=1, device_id={"head": me - 1}, device_id_type=MESH)

    @pl.when(has_right)
    def _():
        pl.semaphore_signal(barrier, inc=1, device_id={"head": me + 1}, device_id_type=MESH)

    pl.semaphore_signal(barrier, inc=1, device_id={"batch": core_peer}, device_id_type=MESH)

    @pl.when(spreads)
    def _():
        for peer in near:
            pl.semaphore_signal(barrier, inc=1, device_id={"batch": peer}, device_id_type=MESH)

    loads = [
        pltpu.make_async_copy(x_hbm, xg.at[me], lsem.at[0]),
        pltpu.make_async_copy(w_hbm, w, lsem.at[1]),
        pltpu.make_async_copy(gate_hbm, gate, lsem.at[1]),
        pltpu.make_async_copy(a_hbm, a32, lsem.at[1]),
        pltpu.make_async_copy(m_hbm, m32, lsem.at[1]),
        pltpu.make_async_copy(
            ow_hbm.at[:, pl.ds(pl.multiple_of(me * cols, cols), cols)], wout.at[me], lsem.at[1]
        ),
        pltpu.make_async_copy(bias_hbm, bias_ref, lsem.at[1]),
        pltpu.make_async_copy(gain_hbm, gain_ref, lsem.at[1]),
    ]
    loads[0].start()

    order = [sorted((j for j in range(n) if j != m), key=lambda j: (abs(j - m), j)) for m in range(n)]
    sources = [select(me, [order[m][k] for m in range(n)]) for k in range(n - 1)]
    span = steps // PIECES

    groups = len(GROUPS)
    width = len(GROUPS[0])
    slots = arrivals(n, groups, width)
    slot_block = [select(me, [slots[m][k][0] for m in range(n)]) for k in range(len(slots[0]))]
    slot_group = [select(me, [slots[m][k][1] for m in range(n)]) for k in range(len(slots[0]))]
    early = max(k + 1 for m in range(n) for k, (_, g) in enumerate(slots[m]) if g == 0)

    def slot_of(j, receiver):
        return j - (j > receiver).astype(jnp.int32)

    def xcopy(side, j, c):
        part = xg.at[j, pl.ds(c * span, span)]
        peer = me + 2 * side - 1
        return pltpu.make_async_remote_copy(
            src_ref=part,
            dst_ref=part,
            send_sem=sent,
            recv_sem=xr.at[slot_of(j, peer), c],
            device_id={"head": peer},
            device_id_type=MESH,
        )

    def landed(part, sem):
        pltpu.make_async_remote_copy(
            src_ref=part,
            dst_ref=part,
            send_sem=sent,
            recv_sem=sem,
            device_id={"head": me},
            device_id_type=MESH,
        ).wait_recv()

    loads[0].wait()
    for load in loads[1:]:
        load.start()
    with jax.named_scope("barrier"):
        pl.semaphore_wait(barrier, has_left.astype(jnp.int32) + has_right.astype(jnp.int32) + 1 + bits * parity)

    @pl.when(has_right)
    def _():
        for c in GROUPS[0]:
            xcopy(1, me, c).start()

    def send_rest():
        for c in range(width, PIECES):
            xcopy(1, me, c).start()

    @pl.when(has_right)
    def _():
        send_rest()

    @pl.when(has_left)
    def _():
        for c in range(PIECES):
            xcopy(0, me, c).start()

    with jax.named_scope("know"):
        for d in range(2, n):

            @pl.when((me >= d - 1) & has_right)
            def _():
                pl.semaphore_signal(know.at[0], inc=1, device_id={"head": me + 1}, device_id_type=MESH)

            @pl.when(me >= d)
            def _():
                pl.semaphore_wait(know.at[0], 1)

        if bits == 2:

            @pl.when(spreads)
            def _():
                pl.semaphore_signal(know.at[2], inc=1, device_id={"batch": near[0]}, device_id_type=MESH)

    def tell_left(d):
        @pl.when((me + d - 1 < n) & has_left)
        def _():
            pl.semaphore_signal(know.at[1], inc=1, device_id={"head": me - 1}, device_id_type=MESH)

    def hear_right(d):
        @pl.when(me + d < n)
        def _():
            pl.semaphore_wait(know.at[1], 1)

    if n > 2:
        tell_left(2)

    def w1copy(j):
        at = pl.ds(pl.multiple_of(chip * slab, slab), slab)
        return pltpu.make_async_remote_copy(
            src_ref=ow_hbm.at[at, pl.ds(pl.multiple_of(j * cols, cols), cols)],
            dst_ref=wout.at[me, at],
            send_sem=sent,
            recv_sem=w1r,
            device_id={"head": j},
            device_id_type=MESH,
        )

    def w2copy(j, peer, sem, rows_sent, begin):
        part = wout.at[j, pl.ds(pl.multiple_of(begin, slab), rows_sent)]
        return pltpu.make_async_remote_copy(
            src_ref=part,
            dst_ref=part,
            send_sem=sent,
            recv_sem=sem,
            device_id={"batch": peer},
            device_id_type=MESH,
        )

    def chip_copies(k, j):
        return [
            w2copy(j, base + 2 * lax.rem(chip + o, chips) + parity, chip_r.at[k], slab, chip * slab)
            for o in range(1, chips)
        ]

    def core_copy(k, j):
        return w2copy(j, core_peer, chip_r.at[k], heads_rows, 0)

    def spread_chips():
        if bits == 2:
            pl.semaphore_wait(know.at[2], 1)
        landed(wout.at[: n - 1, :slab], w1r)
        copies = [chip_copies(k, j) for k, j in enumerate(sources)]
        for o in range(chips - 1):
            for found in copies:
                found[o].start()

    def spread_cores():
        for k, j in enumerate(sources):
            landed(wout.at[j, : (chips - 1) * slab], chip_r.at[k])
            core_copy(k, j).start()

    def project(j, begin, count, first):
        x = xg[j, pl.ds(begin, count)].reshape(count * seqs, feats)
        at = pl.ds(pl.multiple_of(j * feats, feats), feats)
        part = jnp.dot(x, w[at, :], preferred_element_type=F32)
        gpart = jnp.broadcast_to(rowsum(x.astype(F32) * gate[:, at].astype(F32)), (count * seqs, size))
        at = pl.ds(pl.multiple_of(begin * seqs, seqs), count * seqs)
        if first:
            pacc[at, :] = part
            gacc[at, :] = gpart
        else:
            pacc[at, :] += part
            gacc[at, :] += gpart

    def prepare(start, stop):
        for s in range(start, stop):
            ah, al = split(a32[s])
            mh, ml = split(m32[s])
            bt = lax.dot_general(
                jnp.concatenate([ah, al], axis=1),
                jnp.concatenate([mh, mh], axis=1),
                NT,
                preferred_element_type=F32,
            )
            bt = bt + lax.dot_general(ah, ml, NT, preferred_element_type=F32)
            bh, bl = split(bt)
            ab[s, :size, :size] = ah
            ab[s, size:, :size] = al
            ab[s, :size, size:] = bh
            ab[s, size:, size:] = bl

    for j in sources:

        @pl.when(spreads & (j < me))
        def _():
            w1copy(j).start()

    with jax.named_scope("proj0"):
        for load in loads[1:]:
            load.wait()
        project(me, 0, steps, True)
    with jax.named_scope("prepA"):
        prepare(0, seqs)

    def collect(begin, end):
        for k in range(begin, end):
            j, g = slot_block[k], slot_group[k]
            far = has_right & (me - j >= 2)
            held = far & (parity == 1) & (g == groups - 1)
            for at in range(width):
                c = g * width + at
                with jax.named_scope("x%d_%d" % (k, at)):
                    landed(xg.at[j, pl.ds(c * span, span)], xr.at[slot_of(j, me), c])

                @pl.when((j < me) & has_right & jnp.logical_not(held))
                def _():
                    xcopy(1, j, c).start()

                @pl.when((j > me) & has_left)
                def _():
                    xcopy(0, j, c).start()

            @pl.when(held)
            def _():
                with jax.named_scope("t%d" % k):
                    pl.semaphore_wait(turn, 1)
                for c in GROUPS[-1]:
                    xcopy(1, j, c).start()

            with jax.named_scope("p%d" % k):
                project(j, g * width * span, width * span, False)

    past = []
    product = [None]

    def outgoing(part, j, sem):
        return pltpu.make_async_remote_copy(
            src_ref=part,
            dst_ref=part,
            send_sem=sent,
            recv_sem=sem,
            device_id={"head": j},
            device_id_type=MESH,
        )

    def rcopies(j, g):
        sem = rr.at[slot_of(me, j)] if g == groups - 1 else early_r.at[g]
        begin, end = g * width * span * seqs, (g + 1) * width * span * seqs
        return [
            functools.partial(outgoing, rbuf.at[me, pl.ds(begin, end - begin)], j, sem),
            functools.partial(outgoing, sqbuf.at[g, me], j, sem),
        ]

    inner = has_left & has_right
    targets = [jnp.where(inner, sources[k], sources[n - 2 - k]) for k in range(n - 1)]

    def send_readouts(g, begun):
        for k, j in enumerate(targets):
            readout, square = rcopies(j, g)
            if not (begun and k == 0):
                readout().start()
            square().start()

    def advance(g):
        first, last = GROUPS[g][0] * span, (GROUPS[g][-1] + 1) * span
        count = last - first
        half = count * seqs
        at = slice(first * seqs, last * seqs)
        p = pacc[at, :]
        f = 0.8 + 0.2 * jax.nn.sigmoid(gacc[at, :] + bias_ref[...])
        q = p[:, :size]
        k = p[:, size : 2 * size]
        v = p[:, 2 * size :]
        kq[:half, :] = k
        kq[half : 2 * half, :] = q
        for s in range(seqs):
            at = pl.ds(s, 2 * count, stride=seqs)
            hi, lo = split(kq[at, :])
            left = jnp.concatenate([hi.astype(F32), lo.astype(F32)], axis=0).astype(BF16)
            r = jnp.dot(jnp.concatenate([left, left], axis=1), ab[s], preferred_element_type=F32)
            r = r[: 2 * count] + r[2 * count :]
            abuf[at, :] = r[:, :size]
            bbuf[at, :] = r[:, size:]

        def piece(x, t):
            return x[t * seqs : (t + 1) * seqs]

        over_k = lax.rsqrt(rowsum(k * k) + 1e-06)
        over_q = lax.rsqrt(rowsum(q * q) + 1e-06)
        k = k * over_k
        q = q * over_q
        ak = abuf[:half, :] * over_k
        bk = bbuf[:half, :] * over_k
        bq = bbuf[half : 2 * half, :] * over_q
        kt = [piece(k, t) for t in range(count)]
        qt = [piece(q, t) for t in range(count)]
        a = [u for u, _, _, _ in past] + [piece(ak, t) for t in range(count)]
        dots = [[rowsum(a[s] * kt[t]) for s in range(first + t + 1)] for t in range(count)]
        reads = [[rowsum(a[s] * qt[t]) for s in range(first + t + 1)] for t in range(count)]
        pieces = []
        for t in range(count):
            ft = piece(f, t)
            product[0] = ft if product[0] is None else product[0] * ft
            now = first + t
            for s in range(now + 1):
                lower = past[s][1] if s < now else [past[r][2] * dots[t][r] for r in range(now)]
                for r in range(s):
                    dots[t][s] = dots[t][s] - lower[r] * dots[t][r]
                    reads[t][s] = reads[t][s] - lower[r] * reads[t][r]
            weight = 1.0 / (product[0] + dots[t][now])
            value = piece(v, t) - piece(bk, t)
            for s in range(now):
                value = value - dots[t][s] * past[s][3]
            past.append((a[now], [past[r][2] * dots[t][r] for r in range(now)], weight, weight * value))
            total = piece(bq, t)
            for s in range(now + 1):
                total = total + reads[t][s] * past[s][3]
            pieces.append(total)
        ro = jnp.concatenate(pieces, axis=0)
        rbuf[me, first * seqs : last * seqs] = (gain_ref[...] * ro).astype(BF16)
        if g < groups - 1:

            @pl.when(jnp.logical_not(inner))
            def _():
                rcopies(targets[0], g)[0]().start()

        else:
            rcopies(targets[0], g)[0]().start()
        hi, lo = split(ro * ro)
        both = jnp.concatenate([hi, lo], axis=1)
        sqbuf[g, me] = lax.dot_general(
            jnp.ones((8, 2 * size), BF16),
            jnp.concatenate([both] * (rows // half), axis=0),
            NT,
            preferred_element_type=F32,
        )[:1]
        if g < groups - 1:

            @pl.when(jnp.logical_not(inner))
            def _():
                send_readouts(g, True)

        else:
            send_readouts(g, True)

            @pl.when(inner)
            def _():
                for before in range(g):
                    send_readouts(before, False)

    collect(0, 1)
    if n > 2:
        hear_right(2)
        if n > 3:
            tell_left(3)
    collect(1, 2)
    with jax.named_scope("learn"):
        for d in range(3, n):
            hear_right(d)
            if d + 1 < n:
                tell_left(d + 1)

    collect(2, early - 2)
    for j in sources:

        @pl.when(spreads & (me == 0) & (j < n - 1))
        def _():
            w1copy(j).start()

    collect(early - 2, early - 1)

    @pl.when(spreads & (me == 0))
    def _():
        with jax.named_scope("spreadA0"):
            spread_chips()
        w1copy(n - 1).start()

    collect(early - 1, early)

    @pl.when(inner)
    def _():
        collect(early, len(slot_block))

    for j in sources:

        @pl.when(spreads & inner & (j > me) & (j < n - 1))
        def _():
            w1copy(j).start()

    with jax.named_scope("adv0"):
        advance(0)

    for k in range(len(slot_block)):

        @pl.when(has_right & (me - slot_block[k] >= 2) & (parity == 0) & (slot_group[k] == groups - 1))
        def _():
            pl.semaphore_signal(turn, inc=1, device_id={"batch": core_peer}, device_id_type=MESH)

    @pl.when(spreads & inner & (me < n - 2))
    def _():
        w1copy(n - 1).start()

    @pl.when(spreads & inner & (me == n - 2))
    def _():
        w1copy(n - 1).start()

    @pl.when(jnp.logical_not(inner))
    def _():
        collect(early, len(slot_block))

    with jax.named_scope("adv1"):
        advance(1)

    with jax.named_scope("spreadA"):

        @pl.when(spreads & (me > 0))
        def _():
            spread_chips()

    with jax.named_scope("spreadB"):

        @pl.when(spreads)
        def _():
            spread_cores()

    def send_done(part):
        pltpu.make_async_remote_copy(
            src_ref=part,
            dst_ref=part,
            send_sem=sent,
            recv_sem=w1r,
            device_id={"head": me},
            device_id_type=MESH,
        ).wait_send()

    extra = rows * 4 // (size * 2)
    count = width * span * seqs

    def spread_landed(k, j):
        @pl.when(jnp.logical_not(spreads))
        def _():
            landed(wout.at[j], chip_r.at[k])

    def write(part, acc, squares):
        height = part.stop - part.start
        scale = jnp.broadcast_to(squares, (size, rows)).T[:height]
        for at in range(0, cols, size):
            out_ref[part, at : at + size] = acc[:, at : at + size] * scale

    def scale_of(squares):
        return lax.rsqrt(squares / (n * size) + 1e-06)

    def finish(g):
        part = slice(g * count, (g + 1) * count)
        acc = jnp.dot(rbuf[me, part], wout[me], preferred_element_type=F32)
        squares = sqbuf[g, me]
        if g < groups - 1:
            landed(rbuf.at[: n - 1, : count + extra], early_r.at[g])
        for k, j in enumerate(sources):
            if g == 0:
                spread_landed(k, j)
            if g == groups - 1:
                landed(rbuf.at[j, : count + extra], rr.at[slot_of(j, me)])
            acc = acc + jnp.dot(rbuf[j, part], wout[j], preferred_element_type=F32)
            squares = squares + sqbuf[g, j]
        write(part, acc, scale_of(squares))

    def finish_all():
        acc = jnp.dot(rbuf[me], wout[me], preferred_element_type=F32)
        squares = [sqbuf[g, me] for g in range(groups)]
        for g in range(groups - 1):
            landed(rbuf.at[: n - 1, : count + extra], early_r.at[g])
        for j in sources:
            landed(rbuf.at[j, : count + extra], rr.at[slot_of(j, me)])
            squares = [squares[g] + sqbuf[g, j] for g in range(groups)]
        scales = [scale_of(squares[g]) for g in range(groups)]
        for k, j in enumerate(sources):
            spread_landed(k, j)
            acc = acc + jnp.dot(rbuf[j], wout[j], preferred_element_type=F32)
        for g in range(groups):
            part = slice(g * count, (g + 1) * count)
            write(part, acc[part], scales[g])

    def sent_done():
        @pl.when(has_right)
        def _():
            send_done(xg.at[0])

        @pl.when(has_left)
        def _():
            send_done(xg.at[0])

        for j in sources:

            @pl.when(inner)
            def _():
                send_done(xg.at[0])

        for j in sources:
            for copy in rcopies(j, 0):
                copy().wait_send()

    @pl.when(me < n - 1)
    def _():
        for g in range(groups):
            if g == groups - 1:
                sent_done()
            finish(g)

    @pl.when(me == n - 1)
    def _():
        sent_done()
        finish_all()

    @pl.when(spreads)
    def _():
        for _ in sources:
            send_done(wout.at[0, :slab])
            send_done(wout.at[0, : (chips - 1) * slab])
            send_done(wout.at[0])

    for j in sources:
        for copy in rcopies(j, groups - 1):
            copy().wait_send()


def local(n, batch, inputs, in_weight, gate_weight, gate_bias, norm_gain, out_weight, inv_gram, value_key):
    steps, seqs, feats = inputs.shape
    d_model, heads, width = in_weight.shape
    size = width // 3
    rows = steps * seqs
    cols = out_weight.shape[1] // n
    group = math.gcd(math.gcd(batch, 8), out_weight.shape[0] // 16)
    assert heads == 1 and steps % PIECES == 0 and group > 1
    anywhere = pl.BlockSpec(memory_space=pl.ANY)
    vmem = pl.BlockSpec(memory_space=pltpu.VMEM)
    dma = pltpu.SemaphoreType.DMA
    out = pl.pallas_call(
        functools.partial(kernel, n, group),
        out_shape=pltpu.VMEM((rows, cols), F32),
        in_specs=[anywhere] * 8,
        out_specs=vmem,
        scratch_shapes=[
            pltpu.VMEM((1, 1), F32),
            pltpu.VMEM((1, size), F32),
            pltpu.VMEM((n, steps, seqs, feats), BF16),
            pltpu.VMEM((d_model, width), BF16),
            pltpu.VMEM((1, d_model), BF16),
            pltpu.VMEM((seqs, size, size), F32),
            pltpu.VMEM((seqs, size, size), F32),
            pltpu.VMEM((seqs, 2 * size, 2 * size), BF16),
            pltpu.VMEM((n, out_weight.shape[0], cols), BF16),
            pltpu.VMEM((rows, width), F32),
            pltpu.VMEM((rows, size), F32),
            pltpu.VMEM((2 * rows, size), F32),
            pltpu.VMEM((2 * rows, size), F32),
            pltpu.VMEM((2 * rows, size), F32),
            pltpu.VMEM((n, rows, size), BF16),
            pltpu.VMEM((len(GROUPS), n, 1, rows), F32),
            dma((2,)),
            dma((n - 1, PIECES)),
            pltpu.SemaphoreType.REGULAR((3,)),
            pltpu.SemaphoreType.REGULAR,
            dma,
            dma((n - 1,)),
            dma((len(GROUPS) - 1,)),
            dma((n - 1,)),
            dma,
        ],
        compiler_params=pltpu.CompilerParams(collective_id=0, has_side_effects=True),
    )(
        inputs,
        in_weight.reshape(d_model, width),
        gate_weight.reshape(1, d_model),
        gate_bias.reshape(1, 1),
        norm_gain.reshape(1, size),
        out_weight,
        inv_gram.reshape(seqs, size, size),
        value_key.reshape(seqs, size, size),
    )
    return out.reshape(steps, seqs, cols)


def solution(mesh):
    in_specs = (
        P(None, "batch", "head"),
        P(None, "head", None),
        P(None, "head"),
        P("head"),
        P("head"),
        P("head", None),
        P("batch", "head", None, None),
        P("batch", "head", None, None),
    )
    out_specs = P(None, "batch", "head")
    return jax.shard_map(
        functools.partial(local, mesh.shape["head"], mesh.shape["batch"]),
        mesh=mesh,
        in_specs=in_specs,
        out_specs=out_specs,
        check_vma=False,
    )
```
